32 devices in a mesh: comm: 4 (over z), arc: 8 (over y, x, core).
Axes of the slice: x: 2, y: 2, z: 4, core: 2. Of those that a mesh axis runs over, the one named last changes fastest.
Arguments:
- prev_dist: float32 [512, 2048], P('comm', 'arc'), may hold values from 0 to 4
- source_node: int32 [512], P('comm'), may hold values from 0 to 2047, as said below
- arc_tail: int32 [16, 2048], P(None, 'arc'), may hold values from 0 to 2047, as said below
- base_cost: float32 [16, 2048], P(None, 'arc'), may hold values from 0.05 to 1
- arc_price: float32 [16, 2048], P(None, 'arc'), may hold values from 0 to 1
- capacity: float32 [16, 2048], P(None, 'arc')
- path_arcs: int32 [512, 128], P(('comm', 'arc')), may hold values from 0 to 32767, as said below
- demand: float32 [512], P(('comm', 'arc')), may hold values from 0.5 to 2
Outputs:
- final_dist: float32 [512, 2048], P('comm', 'arc')
- new_price: float32 [16, 2048], P(None, 'arc')
The draws below stay inside these ranges and needn't reach their ends.
Inputs may be any that keep to these rules, and one draw needn't show every extreme that they name: `arc_tail`: the tail of arc s * 2048 + v lies in a node block (nodes 128 b to 128 b + 127) at most 2 blocks before or after v's block, counted around the cycle of blocks. Row k is a walk: the head of path_arcs[k, h + 1] (its id modulo 2048) is the tail of path_arcs[k, h]. `source_node`: the tail of path_arcs[k, 127].
All inputs are finite; a program needn't handle non-finite values.
Results may differ from the reference program's by a relative error of at most 0.00002.
Values sent between devices are 32-bit elements; how exact they have to be, the bound alone decides.
No kernel may reach another device: no remote copies, remote signals or barrier semaphores. Data moves between devices by JAX's collectives and lax.ppermute only.
A program may use at most 64 MiB of HBM per device.

```python
import math
import jax
import jax.numpy as jnp
from jax import lax

LANES = 128
BLK_DEV = 2
IN_DEG = 16
SWEEPS = 8
HOPS = 128
NODES = 2048
K = 512


def make_tails(key):
    tail_key = jax.random.fold_in(key, 11)
    key_pair = jax.random.split(tail_key, 2)
    head_nodes = jnp.arange(NODES, dtype=jnp.int32)
    head_block = head_nodes // LANES
    blocks_all = NODES // LANES
    offset = jax.random.randint(key_pair[0], (IN_DEG, NODES), -BLK_DEV, BLK_DEV + 1)
    lane_pick = jax.random.randint(key_pair[1], (IN_DEG, NODES), 0, LANES)
    return (jnp.mod(head_block[None, :] + offset, blocks_all) * LANES + lane_pick).astype(jnp.int32)


def make_walks(key):
    tail_nodes = make_tails(key).reshape(-1)
    walk_key = jax.random.fold_in(key, 23)
    key_pair = jax.random.split(walk_key, 2)
    sink_nodes = jax.random.randint(key_pair[0], (K,), 0, NODES).astype(jnp.int32)
    slot_picks = jax.random.randint(key_pair[1], (HOPS, K), 0, IN_DEG).astype(jnp.int32)

    def advance(current, picked):
        arc_ids = picked * NODES + current
        return (tail_nodes[arc_ids], arc_ids)
    endpoint, walked = lax.scan(advance, sink_nodes, slot_picks)
    return (walked.T.astype(jnp.int32), endpoint.astype(jnp.int32))


def draw_arc_tail(key, part):
    return make_tails(key)


def draw_path_arcs(key, part):
    return make_walks(key)[0]


def draw_source_node(key, part):
    return make_walks(key)[1]


def draw_capacity(key, part):
    mean_load = K * HOPS / (IN_DEG * NODES)
    positions = jnp.arange(NODES, dtype=jnp.float32) / NODES
    rough_factor = jnp.exp(jax.random.uniform(key, (IN_DEG, NODES), jnp.float32, math.log(0.3), math.log(3.0)))
    return (mean_load * rough_factor * (0.5 + 1.5 * positions)[None, :]).astype(jnp.float32)


def block_scale(own_key, dims, pieces, least, largest):
    loudness = 1.0
    for dim, parts in pieces:
        heights = jax.random.uniform(jax.random.fold_in(jax.random.fold_in(own_key, 6), dim), (parts,), jnp.float32, least / len(pieces), largest / len(pieces))
        loudness = loudness * jnp.repeat(jnp.exp(heights), dims[dim] // parts).reshape((-1,) + (1,) * (len(dims) - 1 - dim))
    return loudness


def setup_inputs(seed: int = 0) -> dict:
    key_of = jax.random.split(jax.random.key(seed), 9)
    return {
        "prev_dist": jnp.clip(4.0 * jax.random.uniform(key_of[0], (K, NODES), jnp.float32) ** block_scale(key_of[0], (K, NODES), ((0, 4), (1, 8)), -0.2, 0.2), 0.0, 4.0),
        "source_node": draw_source_node(jax.random.fold_in(key_of[8], 71), 0),
        "arc_tail": draw_arc_tail(jax.random.fold_in(key_of[8], 71), 0),
        "base_cost": jnp.clip(jnp.exp(math.log(1.0) - 2.9957323 * jax.random.uniform(key_of[3], (IN_DEG, NODES), jnp.float32) ** block_scale(key_of[3], (IN_DEG, NODES), ((1, 8),), -0.2, 0.2)), 0.05, 1.0),
        "arc_price": jnp.clip(1.0 * jax.random.uniform(key_of[4], (IN_DEG, NODES), jnp.float32) ** block_scale(key_of[4], (IN_DEG, NODES), ((1, 8),), -0.2, 0.2), 0.0, 1.0),
        "capacity": draw_capacity(jax.random.fold_in(key_of[8], 71), 0),
        "path_arcs": draw_path_arcs(jax.random.fold_in(key_of[8], 71), 0),
        "demand": jnp.clip(jnp.exp(math.log(2.0) - 1.3862944 * jax.random.uniform(key_of[7], (K,), jnp.float32) ** block_scale(key_of[7], (K,), ((0, 32),), -0.2, 0.2)), 0.5, 2.0),
    }


step_size = 0.25
eps_value = 1e-06

def reference(prev_dist, source_node, arc_tail, base_cost, arc_price, capacity, path_arcs, demand):
    arc_weight = base_cost + arc_price
    node_ids = jnp.arange(NODES, dtype=jnp.int32)
    distance = jnp.where(node_ids[None, :] == source_node[:, None], jnp.float32(0.0), prev_dist)
    for sweep_number in range(SWEEPS):
        best_dist = distance
        for in_slot in range(IN_DEG):
            candidate = jnp.take(distance, arc_tail[in_slot], axis=1) + arc_weight[in_slot][None, :]
            best_dist = jnp.minimum(best_dist, candidate)
        distance = best_dist
    amounts = jnp.broadcast_to(demand[:, None], path_arcs.shape).reshape(-1)
    flattened = jnp.zeros((IN_DEG * NODES,), jnp.float32).at[path_arcs.reshape(-1)].add(amounts)
    arc_flow = flattened.reshape(IN_DEG, NODES)
    gradient = arc_flow - capacity
    scale_root = jnp.sqrt(jnp.sum(gradient * gradient) / (IN_DEG * NODES) + eps_value)
    new_price = jnp.maximum(arc_price + step_size * gradient / scale_root, jnp.float32(0.0))
    return (distance, new_price)
```

```python
import functools

import jax
import jax.numpy as jnp
from jax import lax
from jax.experimental import pallas as pl
from jax.experimental.pallas import tpu as pltpu
from jax.sharding import PartitionSpec as P

SWEEPS = 8
REACH = 2
LANES = 128
SUB = 8

step_size = 0.25
eps_value = 1e-06


def vmem_spec():
    return pl.BlockSpec(memory_space=pltpu.VMEM)


def smem_spec():
    return pl.BlockSpec(memory_space=pltpu.SMEM)


def three_parts(x):
    first = x.astype(jnp.bfloat16)
    rest = x - first.astype(jnp.float32)
    second = rest.astype(jnp.bfloat16)
    third = (rest - second.astype(jnp.float32)).astype(jnp.bfloat16)
    return first, second, third


def pack_kernel(
    node_count, demand_ref, dist_ref, tail_ref, cost_ref, price_ref, path_ref, out_ref
):
    peers = out_ref.shape[0]
    degree, shard_nodes = tail_ref.shape
    shard_blocks = shard_nodes // LANES
    mine = dist_ref.shape[0] // peers
    block_total = node_count // LANES
    routes, hops = path_ref.shape

    path = path_ref[...]
    slot = path // node_count
    node = path - slot * node_count
    block = node // LANES
    lane = node - block * LANES
    row = block * degree + slot
    row_total = block_total * degree
    row_ids = lax.broadcasted_iota(jnp.int32, (row_total, hops), 0)
    lane_ids = lax.broadcasted_iota(jnp.int32, (LANES, hops), 0)
    left = [[], [], []]
    right = []
    for k in range(routes):
        hit = row_ids == row[k : k + 1, :]
        amount = jnp.full((1, hops), demand_ref[k], jnp.float32)
        for part, piece in enumerate(three_parts(amount)):
            left[part].append(
                jnp.where(hit, piece.astype(jnp.float32), jnp.float32(0.0)).astype(jnp.bfloat16)
            )
        right.append(
            jnp.where(lane_ids == lane[k : k + 1, :], jnp.float32(1.0), jnp.float32(0.0)).astype(
                jnp.bfloat16
            )
        )
    right = jnp.concatenate(right, axis=1)
    flow = None
    for part in (2, 1, 0):
        term = lax.dot_general(
            jnp.concatenate(left[part], axis=1),
            right,
            (((1,), (1,)), ((), ())),
            preferred_element_type=jnp.float32,
        )
        flow = term if flow is None else flow + term

    tail = tail_ref[...].astype(jnp.float32)
    weight = cost_ref[...] + price_ref[...]
    arc_rows = degree * shard_blocks
    base = mine * shard_blocks
    for j in range(peers):
        for b in range(shard_blocks):
            cols = slice(b * LANES, (b + 1) * LANES)
            out_ref[j, b * mine : (b + 1) * mine, :] = dist_ref[j * mine : (j + 1) * mine, cols]
            out_ref[j, base + b * degree : base + (b + 1) * degree, :] = tail[:, cols]
            start = base + arc_rows + b * degree
            out_ref[j, start : start + degree, :] = weight[:, cols]
        start = base + 2 * arc_rows
        out_ref[j, start : start + arc_rows, :] = flow[j * arc_rows : (j + 1) * arc_rows, :]


def halo_store(ref, k, half, groups, span, value):
    blocks = groups * SUB
    base = k * span + SUB
    ref[base + half * SUB : base + (half + 1) * SUB, :] = value
    if half == groups - 1:
        ref[base - REACH : base, :] = value[SUB - REACH :, :]
    if half == 0:
        ref[base + blocks : base + blocks + REACH, :] = value[:REACH, :]


def unpack_kernel(mine, degree, source_ref, first_ref, buf_ref, x_ref, idx_ref, off_ref, w_ref, flow_ref, stage, stage_idx):
    peers = buf_ref.shape[0]
    span = x_ref.shape[0] // mine
    block_total = span - 2 * SUB
    groups = block_total // SUB
    shard_blocks = block_total // peers
    arc_rows = degree * shard_blocks
    base = mine * shard_blocks
    total = None
    for i in range(peers):
        part = buf_ref[i, base + 2 * arc_rows : base + 3 * arc_rows, :]
        total = part if total is None else total + part
    flow_ref[...] = total
    for i in range(peers):
        for b in range(shard_blocks):
            blk = i * shard_blocks + b
            stage[pl.ds(blk, mine, stride=block_total), :] = buf_ref[i, b * mine : (b + 1) * mine, :]
            s0 = base + b * degree
            stage_idx[pl.ds(blk, degree, stride=block_total), :] = buf_ref[i, s0 : s0 + degree, :]
            s1 = base + arc_rows + b * degree
            w_ref[pl.ds(blk, degree, stride=block_total), :] = buf_ref[i, s1 : s1 + degree, :]
    rows = lax.broadcasted_iota(jnp.int32, (SUB, LANES), 0)
    lanes = lax.broadcasted_iota(jnp.int32, (SUB, LANES), 1)
    first = first_ref[0]
    for half in range(groups):
        node = (rows + half * SUB) * LANES + lanes
        for k in range(mine):
            at = k * block_total + half * SUB
            value = jnp.where(node == source_ref[first + k], jnp.float32(0.0), stage[at : at + SUB, :])
            halo_store(x_ref, k, half, groups, span, value)
        for s in range(degree):
            at = s * block_total + half * SUB
            tail = stage_idx[at : at + SUB, :].astype(jnp.int32)
            tail_block = tail // LANES
            idx_ref[at : at + SUB, :] = tail - tail_block * LANES
            off = tail_block - (rows + half * SUB) + REACH
            off = jnp.where(off < 0, off + block_total, off)
            off_ref[at : at + SUB, :] = jnp.where(off >= block_total, off - block_total, off)


def sweep_once(mine, degree, src, dst, idx_ref, off_ref, w_ref):
    span = src.shape[0] // mine
    block_total = span - 2 * SUB
    groups = block_total // SUB
    for half in range(groups):
        best = [src[k * span + SUB + half * SUB : k * span + SUB + (half + 1) * SUB, :] for k in range(mine)]
        for s in range(degree):
            at = s * block_total + half * SUB
            idx = idx_ref[at : at + SUB, :]
            off = off_ref[at : at + SUB, :]
            w = w_ref[at : at + SUB, :]
            masks = [off == o for o in range(2 * REACH)]
            for k in range(mine):
                base = k * span + SUB + half * SUB - REACH
                picked = None
                for o in reversed(range(2 * REACH + 1)):
                    value = jnp.take_along_axis(
                        src[base + o : base + o + SUB, :], idx, axis=1, mode="promise_in_bounds"
                    )
                    picked = value if picked is None else jnp.where(masks[o], value, picked)
                best[k] = jnp.minimum(best[k], picked + w)
        for k in range(mine):
            halo_store(dst, k, half, groups, span, best[k])


def sweep_kernel(mine, degree, count, x_ref, idx_ref, off_ref, w_ref, out_ref, other):
    span = x_ref.shape[0] // mine
    args = (idx_ref, off_ref, w_ref)
    pairs, odd = divmod(count, 2)
    if odd:
        sweep_once(mine, degree, x_ref, out_ref, *args)
    else:
        out_ref[...] = x_ref[...]
    if pairs:
        @pl.loop(0, pairs)
        def _(_):
            sweep_once(mine, degree, out_ref, other, *args)
            sweep_once(mine, degree, other, out_ref, *args)


def out_kernel(mine, x_ref, flow_ref, cap_ref, out_ref, grad_ref):
    peers = out_ref.shape[0]
    span = x_ref.shape[0] // mine
    block_total = span - 2 * SUB
    shard_blocks = block_total // peers
    degree = cap_ref.shape[0]
    square = None
    for b in range(shard_blocks):
        cols = slice(b * LANES, (b + 1) * LANES)
        grad = flow_ref[b * degree : (b + 1) * degree, :] - cap_ref[:, cols]
        grad_ref[:, cols] = grad
        term = grad * grad
        square = term if square is None else square + term
    folded = jnp.sum(square.reshape(degree // SUB, SUB, LANES), axis=0)
    base = mine * shard_blocks
    for i in range(peers):
        for b in range(shard_blocks):
            blk = SUB + i * shard_blocks + b
            out_ref[i, b * mine : (b + 1) * mine, :] = x_ref[pl.ds(blk, mine, stride=span), :]
        out_ref[i, base : base + SUB, :] = folded


def final_kernel(mine, arc_total, buf_ref, grad_ref, price_ref, dist_ref, new_ref):
    peers = buf_ref.shape[0]
    shard_blocks = dist_ref.shape[1] // LANES
    base = mine * shard_blocks
    total = None
    for i in range(peers):
        for b in range(shard_blocks):
            dist_ref[i * mine : (i + 1) * mine, b * LANES : (b + 1) * LANES] = buf_ref[
                i, b * mine : (b + 1) * mine, :
            ]
        part = buf_ref[i, base : base + SUB, :]
        total = part if total is None else total + part
    square_sum = jnp.sum(jnp.sum(total, axis=1, keepdims=True), axis=0, keepdims=True)
    scale_root = jnp.sqrt(square_sum / arc_total + eps_value)
    new_ref[...] = jnp.maximum(
        price_ref[...] + step_size * grad_ref[...] / scale_root, jnp.float32(0.0)
    )


def comm_sum_parts(sweeps, size):
    steps = max(size.bit_length() - 1, 1)
    return [sweeps // steps + (1 if n < sweeps % steps else 0) for n in range(steps)]


def shards(prev_dist, source_node, arc_tail, base_cost, arc_price, capacity, path_arcs, demand):
    commodities, shard_nodes = prev_dist.shape
    peers = lax.axis_size("arc")
    groups = lax.axis_size("comm")
    node_count = shard_nodes * peers
    degree = arc_tail.shape[0]
    mine = commodities // peers
    shard_blocks = shard_nodes // LANES
    block_total = node_count // LANES
    span = block_total + 2 * SUB
    arc_rows = degree * shard_blocks
    f32, i32 = jnp.float32, jnp.int32
    shape = jax.ShapeDtypeStruct
    v, s = vmem_spec, smem_spec

    packed = pl.pallas_call(
        functools.partial(pack_kernel, node_count),
        out_shape=shape((peers, mine * shard_blocks + 3 * arc_rows, LANES), f32),
        in_specs=[s(), v(), v(), v(), v(), v()],
        out_specs=v(),
        name="pack",
    )(demand, prev_dist, arc_tail, base_cost, arc_price, path_arcs)
    received = lax.all_to_all(packed, "arc", 0, 0, tiled=True)
    first = (lax.axis_index("arc") * mine).astype(i32).reshape(1)
    table = degree * block_total
    x, idx, off, w, flow = pl.pallas_call(
        functools.partial(unpack_kernel, mine, degree),
        out_shape=(
            shape((mine * span, LANES), f32),
            shape((table, LANES), i32),
            shape((table, LANES), i32),
            shape((table, LANES), f32),
            shape((arc_rows, LANES), f32),
        ),
        in_specs=[s(), s(), v()],
        out_specs=(v(), v(), v(), v(), v()),
        scratch_shapes=[
            pltpu.VMEM((mine * block_total, LANES), f32),
            pltpu.VMEM((table, LANES), f32),
        ],
        name="unpack",
    )(source_node, first, received)

    for step, count in enumerate(comm_sum_parts(SWEEPS, groups)):
        distance = 1 << step
        if distance < groups:
            arrived = lax.ppermute(flow, "comm", [(i, i ^ distance) for i in range(groups)])
        x = pl.pallas_call(
            functools.partial(sweep_kernel, mine, degree, count),
            out_shape=shape((mine * span, LANES), f32),
            in_specs=[v(), v(), v(), v()],
            out_specs=v(),
            scratch_shapes=[pltpu.VMEM((mine * span, LANES), f32)],
            name="sweeps",
        )(x, idx, off, w)
        if distance < groups:
            flow = flow + arrived

    back, gradient = pl.pallas_call(
        functools.partial(out_kernel, mine),
        out_shape=(
            shape((peers, mine * shard_blocks + SUB, LANES), f32),
            shape((degree, shard_nodes), f32),
        ),
        in_specs=[v(), v(), v()],
        out_specs=(v(), v()),
        name="give_back",
    )(x, flow, capacity)
    final = lax.all_to_all(back, "arc", 0, 0, tiled=True)
    return pl.pallas_call(
        functools.partial(final_kernel, mine, degree * node_count),
        out_shape=(shape((commodities, shard_nodes), f32), shape((degree, shard_nodes), f32)),
        in_specs=[v(), v(), v()],
        out_specs=(v(), v()),
        name="finish",
    )(final, gradient, arc_price)


def solution(mesh):
    in_specs = (
        P("comm", "arc"),
        P("comm"),
        P(None, "arc"),
        P(None, "arc"),
        P(None, "arc"),
        P(None, "arc"),
        P(("comm", "arc"), None),
        P(("comm", "arc")),
    )
    out_specs = (P("comm", "arc"), P(None, "arc"))
    return jax.shard_map(shards, mesh=mesh, in_specs=in_specs, out_specs=out_specs, check_vma=False)
```

```python
import functools

import jax
import jax.numpy as jnp
from jax import lax
from jax.experimental import pallas as pl
from jax.experimental.pallas import tpu as pltpu
from jax.sharding import PartitionSpec as P

SWEEPS = 8
EARLY_SWEEPS = 2
REACH = 2
LANES = 128
SUB = 8
VMEM_GRANT = 24 * 1024 * 1024

TURNS = ((None, None), (0, 1), (2, 3), (4, 5), (6, 0), (1, 3))

step_size = 0.25
eps_value = 1e-06


def vmem_spec():
    return pl.BlockSpec(memory_space=pltpu.VMEM)


def smem_spec():
    return pl.BlockSpec(memory_space=pltpu.SMEM)


def three_parts(x):
    first = x.astype(jnp.bfloat16)
    rest = x - first.astype(jnp.float32)
    second = rest.astype(jnp.bfloat16)
    third = (rest - second.astype(jnp.float32)).astype(jnp.bfloat16)
    return first, second, third


def pack_kernel(
    node_count, demand_ref, dist_ref, tail_ref, cost_ref, price_ref, path_ref, out_ref
):
    peers = out_ref.shape[0]
    degree, shard_nodes = tail_ref.shape
    shard_blocks = shard_nodes // LANES
    mine = dist_ref.shape[0] // peers
    block_total = node_count // LANES
    routes, hops = path_ref.shape

    path = path_ref[...]
    slot = path // node_count
    node = path - slot * node_count
    block = node // LANES
    lane = node - block * LANES
    row = block * degree + slot
    row_total = block_total * degree
    row_ids = lax.broadcasted_iota(jnp.int32, (row_total, hops), 0)
    lane_ids = lax.broadcasted_iota(jnp.int32, (LANES, hops), 0)
    left = [[], [], []]
    right = []
    for k in range(routes):
        hit = row_ids == row[k : k + 1, :]
        amount = jnp.full((1, hops), demand_ref[k], jnp.float32)
        for part, piece in enumerate(three_parts(amount)):
            left[part].append(
                jnp.where(hit, piece.astype(jnp.float32), jnp.float32(0.0)).astype(jnp.bfloat16)
            )
        right.append(
            jnp.where(lane_ids == lane[k : k + 1, :], jnp.float32(1.0), jnp.float32(0.0)).astype(
                jnp.bfloat16
            )
        )
    right = jnp.concatenate(right, axis=1)
    flow = None
    for part in (2, 1, 0):
        term = lax.dot_general(
            jnp.concatenate(left[part], axis=1),
            right,
            (((1,), (1,)), ((), ())),
            preferred_element_type=jnp.float32,
        )
        flow = term if flow is None else flow + term

    tail = tail_ref[...].astype(jnp.float32)
    weight = cost_ref[...] + price_ref[...]
    arc_rows = degree * shard_blocks
    base = mine * shard_blocks
    for j in range(peers):
        for b in range(shard_blocks):
            cols = slice(b * LANES, (b + 1) * LANES)
            out_ref[j, b * mine : (b + 1) * mine, :] = dist_ref[j * mine : (j + 1) * mine, cols]
            out_ref[j, base + b * degree : base + (b + 1) * degree, :] = tail[:, cols]
            start = base + arc_rows + b * degree
            out_ref[j, start : start + degree, :] = weight[:, cols]
        start = base + 2 * arc_rows
        out_ref[j, start : start + arc_rows, :] = flow[j * arc_rows : (j + 1) * arc_rows, :]


def halo_store(ref, k, half, groups, span, value):
    blocks = groups * SUB
    base = k * span + SUB
    ref[base + half * SUB : base + (half + 1) * SUB, :] = value
    if half == groups - 1:
        ref[base - REACH : base, :] = value[SUB - REACH :, :]
    if half == 0:
        ref[base + blocks : base + blocks + REACH, :] = value[:REACH, :]


def flow_kernel(rows, buf_ref, flow_ref):
    total = None
    for i in range(buf_ref.shape[0]):
        part = buf_ref[i, buf_ref.shape[1] - rows :, :]
        total = part if total is None else total + part
    flow_ref[...] = total


def plan_rounds(degree, block_total, half, stage, idx_ref, w_ref, left_idx_ref, left_off_ref, left_w_ref):
    groups = block_total // SUB
    width = 2 * REACH + 1
    rows = lax.broadcasted_iota(jnp.int32, (SUB, LANES), 0) + half * SUB
    used = jnp.zeros((SUB, LANES), jnp.int32)
    over = jnp.full((SUB, LANES), degree, jnp.int32)
    lanes_of, weights, bits = [], [], []
    for s in range(degree):
        at = s * block_total + half * SUB
        tail = stage[at : at + SUB, :].astype(jnp.int32)
        block = tail // LANES
        lane = tail - block * LANES
        off = block - rows + REACH
        off = jnp.where(off < 0, off + block_total, off)
        off = jnp.where(off >= block_total, off - block_total, off)
        weight = w_ref[at : at + SUB, :]
        turned = [jnp.left_shift(1, off)]
        for _ in range(3):
            last = turned[-1]
            turned.append(((last << 1) | (last >> (width - 1))) & (2**width - 1))
        open_rounds = jnp.zeros_like(used)
        for j, (low, high) in enumerate(TURNS):
            if low is None:
                spot = turned[0]
            else:
                by_low = ((lane >> low) & 1) == 1
                by_high = ((lane >> high) & 1) == 1
                spot = jnp.where(
                    by_high,
                    jnp.where(by_low, turned[3], turned[2]),
                    jnp.where(by_low, turned[1], turned[0]),
                )
            open_rounds = open_rounds | (spot << (width * j))
        open_rounds = open_rounds & ~used
        bit = open_rounds & -open_rounds
        used = used | bit
        lost = bit == 0
        over = jnp.minimum(over, jnp.where(lost, s, degree))
        left_idx_ref[at : at + SUB, :] = lane
        left_off_ref[at : at + SUB, :] = off
        left_w_ref[at : at + SUB, :] = jnp.where(lost, weight, jnp.float32(jnp.inf))
        lanes_of.append(lane)
        weights.append(weight)
        bits.append(bit)
    for r in range(width * len(TURNS)):
        idx = jnp.zeros((SUB, LANES), jnp.int32)
        weight = jnp.full((SUB, LANES), jnp.inf, jnp.float32)
        for s in range(degree):
            hit = bits[s] == (1 << r)
            idx = jnp.where(hit, lanes_of[s], idx)
            weight = jnp.where(hit, weights[s], weight)
        at = (r * groups + half) * SUB
        idx_ref[at : at + SUB, :] = idx
        w_ref[degree * block_total + at : degree * block_total + at + SUB, :] = weight
    return over


def sweep_once(mine, degree, first_over, src, dst, tables):
    idx_ref, w_ref, left_idx_ref, left_off_ref, left_w_ref = tables
    span = src.shape[0] // mine
    block_total = span - 2 * SUB
    groups = block_total // SUB
    width = 2 * REACH + 1
    w_base = degree * block_total
    lane = lax.broadcasted_iota(jnp.int32, (SUB, LANES), 1)
    bit_masks = [((lane >> t) & 1) == 1 for t in range(LANES.bit_length() - 1)]
    for half in range(groups):
        best = [src[k * span + SUB + half * SUB : k * span + SUB + (half + 1) * SUB, :] for k in range(mine)]
        for j, (low, high) in enumerate(TURNS):
            for q in range(width):
                at = ((j * width + q) * groups + half) * SUB
                idx = idx_ref[at : at + SUB, :]
                w = w_ref[w_base + at : w_base + at + SUB, :]
                for k in range(mine):
                    base = k * span + SUB + half * SUB - REACH

                    def block(turned):
                        o = base + (q - turned) % width
                        return src[o : o + SUB, :]

                    if low is None:
                        shown = block(0)
                    else:
                        shown = jnp.where(
                            bit_masks[high],
                            jnp.where(bit_masks[low], block(3), block(2)),
                            jnp.where(bit_masks[low], block(1), block(0)),
                        )
                    value = jnp.take_along_axis(shown, idx, axis=1, mode="promise_in_bounds")
                    best[k] = jnp.minimum(best[k], value + w)
        for k in range(mine):
            halo_store(dst, k, half, groups, span, best[k])

    @pl.loop(first_over, degree)
    def _(s):
        for half in range(groups):
            at = pl.multiple_of(s * block_total + half * SUB, SUB)
            idx = left_idx_ref[pl.ds(at, SUB), :]
            off = left_off_ref[pl.ds(at, SUB), :]
            w = left_w_ref[pl.ds(at, SUB), :]
            for k in range(mine):
                base = k * span + SUB + half * SUB
                picked = None
                for o in range(width):
                    start = base + o - REACH
                    value = jnp.take_along_axis(
                        src[start : start + SUB, :], idx, axis=1, mode="promise_in_bounds"
                    )
                    picked = value if picked is None else jnp.where(off == o, value, picked)
                now = dst[base : base + SUB, :]
                halo_store(dst, k, half, groups, span, jnp.minimum(now, picked + w))


def sweep_pairs(count, mine, degree, first_over, one, two, tables):
    @pl.loop(0, count // 2)
    def _(_):
        sweep_once(mine, degree, first_over, one, two, tables)
        sweep_once(mine, degree, first_over, two, one, tables)


def begin_kernel(
    mine, degree, count, source_ref, first_ref, buf_ref,
    x_ref, idx_ref, w_ref, left_idx_ref, left_off_ref, left_w_ref, over_ref,
    stage, stage_tail, other,
):
    peers = buf_ref.shape[0]
    span = x_ref.shape[0] // mine
    block_total = span - 2 * SUB
    groups = block_total // SUB
    shard_blocks = block_total // peers
    arc_rows = degree * shard_blocks
    base = mine * shard_blocks
    for i in range(peers):
        for b in range(shard_blocks):
            blk = i * shard_blocks + b
            stage[pl.ds(blk, mine, stride=block_total), :] = buf_ref[i, b * mine : (b + 1) * mine, :]
            s0 = base + b * degree
            stage_tail[pl.ds(blk, degree, stride=block_total), :] = buf_ref[i, s0 : s0 + degree, :]
            s1 = base + arc_rows + b * degree
            w_ref[pl.ds(blk, degree, stride=block_total), :] = buf_ref[i, s1 : s1 + degree, :]
    rows = lax.broadcasted_iota(jnp.int32, (SUB, LANES), 0)
    lanes = lax.broadcasted_iota(jnp.int32, (SUB, LANES), 1)
    first = first_ref[0]
    over = None
    for half in range(groups):
        node = (rows + half * SUB) * LANES + lanes
        for k in range(mine):
            at = k * block_total + half * SUB
            value = jnp.where(node == source_ref[first + k], jnp.float32(0.0), stage[at : at + SUB, :])
            halo_store(x_ref, k, half, groups, span, value)
        part = plan_rounds(
            degree, block_total, half, stage_tail, idx_ref, w_ref,
            left_idx_ref, left_off_ref, left_w_ref,
        )
        over = part if over is None else jnp.minimum(over, part)
    first_over = jnp.min(over.astype(jnp.float32)).astype(jnp.int32)
    over_ref[0] = first_over
    tables = (idx_ref, w_ref, left_idx_ref, left_off_ref, left_w_ref)
    sweep_pairs(count, mine, degree, first_over, x_ref, other, tables)


def end_kernel(
    mine, degree, count, parts, over_ref, start_ref, idx_ref, w_ref, left_idx_ref, left_off_ref,
    left_w_ref, cap_ref, *refs,
):
    flow_refs, (out_ref, grad_ref, x_ref, other) = refs[:parts], refs[parts:]
    peers = out_ref.shape[0]
    span = x_ref.shape[0] // mine
    block_total = span - 2 * SUB
    shard_blocks = block_total // peers
    tables = (idx_ref, w_ref, left_idx_ref, left_off_ref, left_w_ref)
    first_over = over_ref[0]
    sweep_once(mine, degree, first_over, start_ref, other, tables)
    sweep_once(mine, degree, first_over, other, x_ref, tables)
    sweep_pairs(count - 2, mine, degree, first_over, x_ref, other, tables)
    square = None
    for b in range(shard_blocks):
        cols = slice(b * LANES, (b + 1) * LANES)
        flow = None
        for ref in flow_refs:
            part = ref[b * degree : (b + 1) * degree, :]
            flow = part if flow is None else flow + part
        grad = flow - cap_ref[:, cols]
        grad_ref[:, cols] = grad
        term = grad * grad
        square = term if square is None else square + term
    folded = jnp.sum(square.reshape(degree // SUB, SUB, LANES), axis=0)
    base = mine * shard_blocks
    for i in range(peers):
        for b in range(shard_blocks):
            blk = SUB + i * shard_blocks + b
            out_ref[i, b * mine : (b + 1) * mine, :] = x_ref[pl.ds(blk, mine, stride=span), :]
        out_ref[i, base : base + SUB, :] = folded


def final_kernel(mine, arc_total, buf_ref, grad_ref, price_ref, dist_ref, new_ref):
    peers = buf_ref.shape[0]
    shard_blocks = dist_ref.shape[1] // LANES
    base = mine * shard_blocks
    total = None
    for i in range(peers):
        for b in range(shard_blocks):
            dist_ref[i * mine : (i + 1) * mine, b * LANES : (b + 1) * LANES] = buf_ref[
                i, b * mine : (b + 1) * mine, :
            ]
        part = buf_ref[i, base : base + SUB, :]
        total = part if total is None else total + part
    square_sum = jnp.sum(jnp.sum(total, axis=1, keepdims=True), axis=0, keepdims=True)
    scale_root = jnp.sqrt(square_sum / arc_total + eps_value)
    new_ref[...] = jnp.maximum(
        price_ref[...] + step_size * grad_ref[...] / scale_root, jnp.float32(0.0)
    )


def shards(prev_dist, source_node, arc_tail, base_cost, arc_price, capacity, path_arcs, demand):
    commodities, shard_nodes = prev_dist.shape
    peers = lax.axis_size("arc")
    groups = lax.axis_size("comm")
    node_count = shard_nodes * peers
    degree = arc_tail.shape[0]
    mine = commodities // peers
    shard_blocks = shard_nodes // LANES
    block_total = node_count // LANES
    span = block_total + 2 * SUB
    arc_rows = degree * shard_blocks
    f32, i32 = jnp.float32, jnp.int32
    shape = jax.ShapeDtypeStruct
    near = pltpu.VMEM
    v, s = vmem_spec, smem_spec

    def held(x):
        return pltpu.with_memory_space_constraint(x, pltpu.VMEM)

    packed = pl.pallas_call(
        functools.partial(pack_kernel, node_count),
        out_shape=near((peers, mine * shard_blocks + 3 * arc_rows, LANES), f32),
        in_specs=[s(), v(), v(), v(), v(), v()],
        out_specs=v(),
        compiler_params=pltpu.CompilerParams(vmem_limit_bytes=VMEM_GRANT),
        name="pack",
    )(demand, prev_dist, arc_tail, base_cost, arc_price, path_arcs)
    received = held(lax.all_to_all(packed, "arc", 0, 0, tiled=True))

    flow = pl.pallas_call(
        functools.partial(flow_kernel, arc_rows),
        out_shape=near((arc_rows, LANES), f32),
        in_specs=[v()],
        out_specs=v(),
        compiler_params=pltpu.CompilerParams(vmem_limit_bytes=VMEM_GRANT),
        name="flow",
    )(received)
    flows = [flow]
    for d in range(1, groups):
        flows.append(lax.ppermute(flow, "comm", [(i, (i + d) % groups) for i in range(groups)]))

    first = (lax.axis_index("arc") * mine).astype(i32).reshape(1)
    rounds = (2 * REACH + 1) * len(TURNS)
    table = degree * block_total
    state = (mine * span, LANES)
    *tables, over = pl.pallas_call(
        functools.partial(begin_kernel, mine, degree, EARLY_SWEEPS),
        out_shape=(
            near(state, f32),
            near((rounds * block_total, LANES), i32),
            near((table + rounds * block_total, LANES), f32),
            near((table, LANES), i32),
            near((table, LANES), i32),
            near((table, LANES), f32),
            shape((1,), i32),
        ),
        in_specs=[s(), s(), v()],
        out_specs=(v(), v(), v(), v(), v(), v(), s()),
        scratch_shapes=[
            pltpu.VMEM((mine * block_total, LANES), f32),
            pltpu.VMEM((table, LANES), f32),
            pltpu.VMEM(state, f32),
        ],
        compiler_params=pltpu.CompilerParams(vmem_limit_bytes=VMEM_GRANT),
        name="begin",
    )(source_node, first, received)

    back, gradient = pl.pallas_call(
        functools.partial(end_kernel, mine, degree, SWEEPS - EARLY_SWEEPS, groups),
        out_shape=(
            near((peers, mine * shard_blocks + SUB, LANES), f32),
            near((degree, shard_nodes), f32),
        ),
        in_specs=[s()] + [v()] * (len(tables) + 1 + groups),
        out_specs=(v(), v()),
        scratch_shapes=[pltpu.VMEM(state, f32), pltpu.VMEM(state, f32)],
        compiler_params=pltpu.CompilerParams(vmem_limit_bytes=VMEM_GRANT),
        name="end",
    )(over, *map(held, tables), capacity, *map(held, flows))
    final = held(lax.all_to_all(back, "arc", 0, 0, tiled=True))
    return pl.pallas_call(
        functools.partial(final_kernel, mine, degree * node_count),
        out_shape=(shape((commodities, shard_nodes), f32), shape((degree, shard_nodes), f32)),
        in_specs=[v(), v(), v()],
        out_specs=(v(), v()),
        compiler_params=pltpu.CompilerParams(vmem_limit_bytes=VMEM_GRANT),
        name="finish",
    )(final, held(gradient), arc_price)


def solution(mesh):
    in_specs = (
        P("comm", "arc"),
        P("comm"),
        P(None, "arc"),
        P(None, "arc"),
        P(None, "arc"),
        P(None, "arc"),
        P(("comm", "arc"), None),
        P(("comm", "arc")),
    )
    out_specs = (P("comm", "arc"), P(None, "arc"))
    return jax.shard_map(shards, mesh=mesh, in_specs=in_specs, out_specs=out_specs, check_vma=False)
```

```python
import functools

import jax
import jax.numpy as jnp
from jax import lax
from jax.experimental import pallas as pl
from jax.experimental.pallas import tpu as pltpu
from jax.sharding import PartitionSpec as P

SWEEPS = 8
REACH = 2
LANES = 128
SUB = 8
VMEM_GRANT = 24 * 1024 * 1024

TURNS = ((None, None), (0, 1), (2, 3), (4, 5), (6, 0))

step_size = 0.25
eps_value = 1e-06


def vmem_spec():
    return pl.BlockSpec(memory_space=pltpu.VMEM)


def smem_spec():
    return pl.BlockSpec(memory_space=pltpu.SMEM)


def three_parts(x):
    first = x.astype(jnp.bfloat16)
    rest = x - first.astype(jnp.float32)
    second = rest.astype(jnp.bfloat16)
    third = (rest - second.astype(jnp.float32)).astype(jnp.bfloat16)
    return first, second, third


def fetch(pairs, sems):
    copies = [pltpu.make_async_copy(src, dst, sems.at[n]) for n, (src, dst) in enumerate(pairs)]
    for copy in copies:
        copy.start()
    return copies


def pack_kernel(
    node_count, path_hbm, demand_hbm, tail_hbm, cost_hbm, price_hbm, dist_hbm, out_ref,
    path_ref, demand_ref, tail_ref, cost_ref, price_ref, dist_ref, sems,
):
    copies = fetch(
        (
            (path_hbm, path_ref),
            (demand_hbm, demand_ref),
            (tail_hbm, tail_ref),
            (cost_hbm, cost_ref),
            (price_hbm, price_ref),
            (dist_hbm, dist_ref),
        ),
        sems,
    )
    peers = out_ref.shape[0]
    degree, shard_nodes = tail_ref.shape
    shard_blocks = shard_nodes // LANES
    mine = dist_ref.shape[0] // peers
    block_total = node_count // LANES
    routes, hops = path_ref.shape

    copies[0].wait()
    copies[1].wait()
    path = path_ref[...]
    slot = path // node_count
    node = path - slot * node_count
    block = node // LANES
    lane = node - block * LANES
    row = block * degree + slot
    row_total = block_total * degree
    row_ids = lax.broadcasted_iota(jnp.int32, (row_total, hops), 0)
    lane_ids = lax.broadcasted_iota(jnp.int32, (LANES, hops), 0)
    left = [[], [], []]
    right = []
    for k in range(routes):
        hit = row_ids == row[k : k + 1, :]
        amount = jnp.full((1, hops), demand_ref[k], jnp.float32)
        for part, piece in enumerate(three_parts(amount)):
            left[part].append(
                jnp.where(hit, piece.astype(jnp.float32), jnp.float32(0.0)).astype(jnp.bfloat16)
            )
        right.append(
            jnp.where(lane_ids == lane[k : k + 1, :], jnp.float32(1.0), jnp.float32(0.0)).astype(
                jnp.bfloat16
            )
        )
    right = jnp.concatenate(right, axis=1)
    flow = None
    for part in (2, 1, 0):
        term = lax.dot_general(
            jnp.concatenate(left[part], axis=1),
            right,
            (((1,), (1,)), ((), ())),
            preferred_element_type=jnp.float32,
        )
        flow = term if flow is None else flow + term

    for copy in copies[2:]:
        copy.wait()
    tail = tail_ref[...].astype(jnp.float32)
    weight = cost_ref[...] + price_ref[...]
    arc_rows = degree * shard_blocks
    base = mine * shard_blocks
    for j in range(peers):
        for b in range(shard_blocks):
            cols = slice(b * LANES, (b + 1) * LANES)
            out_ref[j, b * mine : (b + 1) * mine, :] = dist_ref[j * mine : (j + 1) * mine, cols]
            out_ref[j, base + b * degree : base + (b + 1) * degree, :] = tail[:, cols]
            start = base + arc_rows + b * degree
            out_ref[j, start : start + degree, :] = weight[:, cols]
        start = base + 2 * arc_rows
        out_ref[j, start : start + arc_rows, :] = flow[j * arc_rows : (j + 1) * arc_rows, :]


def halo_store(ref, k, half, groups, span, value):
    blocks = groups * SUB
    base = k * span + SUB
    ref[base + half * SUB : base + (half + 1) * SUB, :] = value
    if half == groups - 1:
        ref[base - REACH : base, :] = value[SUB - REACH :, :]
    if half == 0:
        ref[base + blocks : base + blocks + REACH, :] = value[:REACH, :]


def flow_kernel(rows, buf_ref, flow_ref):
    total = None
    for i in range(buf_ref.shape[0]):
        part = buf_ref[i, buf_ref.shape[1] - rows :, :]
        total = part if total is None else total + part
    flow_ref[...] = total


def plan_rounds(degree, block_total, half, stage, idx_ref, w_ref, left_idx_ref, left_off_ref, left_w_ref):
    groups = block_total // SUB
    width = 2 * REACH + 1
    rows = lax.broadcasted_iota(jnp.int32, (SUB, LANES), 0) + half * SUB
    used = jnp.zeros((SUB, LANES), jnp.int32)
    over = jnp.full((SUB, LANES), degree, jnp.int32)
    lanes_of, weights, bits, opens, offs = [], [], [], [], []
    for s in range(degree):
        at = s * block_total + half * SUB
        tail = stage[at : at + SUB, :].astype(jnp.int32)
        block = tail // LANES
        lane = tail - block * LANES
        off = block - rows + REACH
        off = jnp.where(off < 0, off + block_total, off)
        off = jnp.where(off >= block_total, off - block_total, off)
        weight = w_ref[at : at + SUB, :]
        turned = [jnp.left_shift(1, off)]
        for _ in range(3):
            last = turned[-1]
            turned.append(((last << 1) | (last >> (width - 1))) & (2**width - 1))
        open_rounds = jnp.zeros_like(used)
        for j, (low, high) in enumerate(TURNS):
            if low is None:
                spot = turned[0]
            else:
                by_low = ((lane >> low) & 1) == 1
                by_high = ((lane >> high) & 1) == 1
                spot = jnp.where(
                    by_high,
                    jnp.where(by_low, turned[3], turned[2]),
                    jnp.where(by_low, turned[1], turned[0]),
                )
            open_rounds = open_rounds | (spot << (width * j))
        free = open_rounds & ~used
        bit = free & -free
        if s >= len(TURNS):
            movable = jnp.zeros_like(used)
            targets = []
            for earlier, taken in zip(opens, bits):
                target = earlier & ~used
                targets.append(target)
                movable = movable | jnp.where(target != 0, taken, 0)
            wanted = open_rounds & movable
            wanted = jnp.where(bit == 0, wanted & -wanted, 0)
            for e, (target, taken) in enumerate(zip(targets, bits)):
                moved = (taken & wanted) != 0
                target = jnp.where(moved, target & -target, 0)
                used = used | target
                bits[e] = jnp.where(moved, target, taken)
            bit = bit | wanted
        used = used | bit
        over = jnp.minimum(over, jnp.where(bit == 0, s, degree))
        opens.append(open_rounds)
        offs.append(off)
        lanes_of.append(lane)
        weights.append(weight)
        bits.append(bit)
    for s in range(degree):
        at = s * block_total + half * SUB
        left_idx_ref[at : at + SUB, :] = lanes_of[s]
        left_off_ref[at : at + SUB, :] = offs[s]
        left_w_ref[at : at + SUB, :] = jnp.where(bits[s] == 0, weights[s], jnp.float32(jnp.inf))
    for r in range(width * len(TURNS)):
        idx = jnp.zeros((SUB, LANES), jnp.int32)
        weight = jnp.full((SUB, LANES), jnp.inf, jnp.float32)
        for s in range(degree):
            hit = bits[s] == (1 << r)
            idx = jnp.where(hit, lanes_of[s], idx)
            weight = jnp.where(hit, weights[s], weight)
        at = (r * groups + half) * SUB
        idx_ref[at : at + SUB, :] = idx
        w_ref[degree * block_total + at : degree * block_total + at + SUB, :] = weight
    return over


def sweep_once(mine, degree, first_over, src, dst, tables):
    idx_ref, w_ref, left_idx_ref, left_off_ref, left_w_ref = tables
    span = src.shape[0] // mine
    block_total = span - 2 * SUB
    groups = block_total // SUB
    width = 2 * REACH + 1
    w_base = degree * block_total
    lane = lax.broadcasted_iota(jnp.int32, (SUB, LANES), 1)
    bit_masks = [((lane >> t) & 1) == 1 for t in range(LANES.bit_length() - 1)]
    for half in range(groups):
        best = [src[k * span + SUB + half * SUB : k * span + SUB + (half + 1) * SUB, :] for k in range(mine)]
        for j, (low, high) in enumerate(TURNS):
            for q in range(width):
                at = ((j * width + q) * groups + half) * SUB
                idx = idx_ref[at : at + SUB, :]
                w = w_ref[w_base + at : w_base + at + SUB, :]
                for k in range(mine):
                    base = k * span + SUB + half * SUB - REACH

                    def block(turned):
                        o = base + (q - turned) % width
                        return src[o : o + SUB, :]

                    if low is None:
                        shown = block(0)
                    else:
                        shown = jnp.where(
                            bit_masks[high],
                            jnp.where(bit_masks[low], block(3), block(2)),
                            jnp.where(bit_masks[low], block(1), block(0)),
                        )
                    value = jnp.take_along_axis(shown, idx, axis=1, mode="promise_in_bounds")
                    best[k] = jnp.minimum(best[k], value + w)
        for k in range(mine):
            halo_store(dst, k, half, groups, span, best[k])

    @pl.loop(first_over, degree)
    def _(s):
        for half in range(groups):
            at = pl.multiple_of(s * block_total + half * SUB, SUB)
            idx = left_idx_ref[pl.ds(at, SUB), :]
            off = left_off_ref[pl.ds(at, SUB), :]
            w = left_w_ref[pl.ds(at, SUB), :]
            for k in range(mine):
                base = k * span + SUB + half * SUB
                picked = None
                for o in range(width):
                    start = base + o - REACH
                    value = jnp.take_along_axis(
                        src[start : start + SUB, :], idx, axis=1, mode="promise_in_bounds"
                    )
                    picked = value if picked is None else jnp.where(off == o, value, picked)
                now = dst[base : base + SUB, :]
                halo_store(dst, k, half, groups, span, jnp.minimum(now, picked + w))


def sweep_pairs(count, mine, degree, first_over, one, two, tables):
    @pl.loop(0, count // 2)
    def _(_):
        sweep_once(mine, degree, first_over, one, two, tables)
        sweep_once(mine, degree, first_over, two, one, tables)


def begin_kernel(
    mine, degree, source_hbm, buf_ref,
    x_ref, idx_ref, w_ref, left_idx_ref, left_off_ref, left_w_ref, over_ref,
    stage, stage_tail, source_ref, sems,
):
    (copy,) = fetch(((source_hbm, source_ref),), sems)
    peers = buf_ref.shape[0]
    span = x_ref.shape[0] // mine
    block_total = span - 2 * SUB
    groups = block_total // SUB
    shard_blocks = block_total // peers
    arc_rows = degree * shard_blocks
    base = mine * shard_blocks
    for i in range(peers):
        for b in range(shard_blocks):
            blk = i * shard_blocks + b
            stage[pl.ds(blk, mine, stride=block_total), :] = buf_ref[i, b * mine : (b + 1) * mine, :]
            s0 = base + b * degree
            stage_tail[pl.ds(blk, degree, stride=block_total), :] = buf_ref[i, s0 : s0 + degree, :]
            s1 = base + arc_rows + b * degree
            w_ref[pl.ds(blk, degree, stride=block_total), :] = buf_ref[i, s1 : s1 + degree, :]
    over = None
    for half in range(groups):
        part = plan_rounds(
            degree, block_total, half, stage_tail, idx_ref, w_ref,
            left_idx_ref, left_off_ref, left_w_ref,
        )
        over = part if over is None else jnp.minimum(over, part)
    over_ref[0] = jnp.min(over.astype(jnp.float32)).astype(jnp.int32)
    copy.wait()
    rows = lax.broadcasted_iota(jnp.int32, (SUB, LANES), 0)
    lanes = lax.broadcasted_iota(jnp.int32, (SUB, LANES), 1)
    first = lax.axis_index("arc") * mine
    for half in range(groups):
        node = (rows + half * SUB) * LANES + lanes
        for k in range(mine):
            at = k * block_total + half * SUB
            value = jnp.where(node == source_ref[first + k], jnp.float32(0.0), stage[at : at + SUB, :])
            halo_store(x_ref, k, half, groups, span, value)


def add_kernel(a_ref, b_ref, out_ref):
    out_ref[...] = a_ref[...] + b_ref[...]


def middle_kernel(
    mine, degree, count, over_ref, start_ref, idx_ref, w_ref, left_idx_ref, left_off_ref,
    left_w_ref, x_ref, other,
):
    x_ref[...] = start_ref[...]
    tables = (idx_ref, w_ref, left_idx_ref, left_off_ref, left_w_ref)
    sweep_pairs(count, mine, degree, over_ref[0], x_ref, other, tables)


def end_kernel(
    mine, degree, count, parts, over_ref, start_ref, idx_ref, w_ref, left_idx_ref, left_off_ref,
    left_w_ref, cap_ref, *refs,
):
    flow_refs, (out_ref, grad_ref, x_ref, other) = refs[:parts], refs[parts:]
    peers = out_ref.shape[0]
    span = x_ref.shape[0] // mine
    block_total = span - 2 * SUB
    shard_blocks = block_total // peers
    tables = (idx_ref, w_ref, left_idx_ref, left_off_ref, left_w_ref)
    first_over = over_ref[0]
    x_ref[...] = start_ref[...]
    sweep_pairs(count, mine, degree, first_over, x_ref, other, tables)
    square = None
    for b in range(shard_blocks):
        cols = slice(b * LANES, (b + 1) * LANES)
        flow = None
        for ref in flow_refs:
            part = ref[b * degree : (b + 1) * degree, :]
            flow = part if flow is None else flow + part
        grad = flow - cap_ref[:, cols]
        grad_ref[:, cols] = grad
        term = grad * grad
        square = term if square is None else square + term
    folded = jnp.sum(square.reshape(degree // SUB, SUB, LANES), axis=0)
    base = mine * shard_blocks
    for i in range(peers):
        for b in range(shard_blocks):
            blk = SUB + i * shard_blocks + b
            out_ref[i, b * mine : (b + 1) * mine, :] = x_ref[pl.ds(blk, mine, stride=span), :]
        out_ref[i, base : base + SUB, :] = folded


def final_kernel(mine, arc_total, buf_ref, grad_ref, price_ref, dist_ref, new_ref):
    peers = buf_ref.shape[0]
    shard_blocks = dist_ref.shape[1] // LANES
    base = mine * shard_blocks
    total = None
    for i in range(peers):
        for b in range(shard_blocks):
            dist_ref[i * mine : (i + 1) * mine, b * LANES : (b + 1) * LANES] = buf_ref[
                i, b * mine : (b + 1) * mine, :
            ]
        part = buf_ref[i, base : base + SUB, :]
        total = part if total is None else total + part
    square_sum = jnp.sum(jnp.sum(total, axis=1, keepdims=True), axis=0, keepdims=True)
    scale_root = jnp.sqrt(square_sum / arc_total + eps_value)
    new_ref[...] = jnp.maximum(
        price_ref[...] + step_size * grad_ref[...] / scale_root, jnp.float32(0.0)
    )


def shards(prev_dist, source_node, arc_tail, base_cost, arc_price, capacity, path_arcs, demand):
    commodities, shard_nodes = prev_dist.shape
    peers = lax.axis_size("arc")
    groups = lax.axis_size("comm")
    node_count = shard_nodes * peers
    degree = arc_tail.shape[0]
    mine = commodities // peers
    shard_blocks = shard_nodes // LANES
    block_total = node_count // LANES
    span = block_total + 2 * SUB
    arc_rows = degree * shard_blocks
    f32, i32 = jnp.float32, jnp.int32
    shape = jax.ShapeDtypeStruct
    near = pltpu.VMEM
    v, s = vmem_spec, smem_spec

    def held(x):
        return pltpu.with_memory_space_constraint(x, pltpu.VMEM)

    def far(x):
        return pltpu.with_memory_space_constraint(x, pltpu.HBM)

    def scratch(*arrays):
        return [pltpu.VMEM(x.shape, x.dtype) for x in arrays]

    h = functools.partial(pl.BlockSpec, memory_space=pltpu.HBM)
    params = pltpu.CompilerParams(vmem_limit_bytes=VMEM_GRANT)
    arcs = (arc_tail, base_cost, arc_price, prev_dist)
    packed = pl.pallas_call(
        functools.partial(pack_kernel, node_count),
        out_shape=near((peers, mine * shard_blocks + 3 * arc_rows, LANES), f32),
        in_specs=[h()] * 6,
        out_specs=v(),
        scratch_shapes=[
            *scratch(path_arcs),
            pltpu.SMEM(demand.shape, f32),
            *scratch(*arcs),
            pltpu.SemaphoreType.DMA((6,)),
        ],
        compiler_params=params,
        name="pack",
    )(far(path_arcs), far(demand), *map(far, arcs))
    received = held(lax.all_to_all(packed, "arc", 0, 0, tiled=True))

    flow = pl.pallas_call(
        functools.partial(flow_kernel, arc_rows),
        out_shape=near((arc_rows, LANES), f32),
        in_specs=[v()],
        out_specs=v(),
        compiler_params=params,
        name="flow",
    )(received)

    def exchange(step):
        pairs = [(i, i ^ (1 << step)) for i in range(groups)]
        return held(lax.ppermute(flow, "comm", pairs))

    steps = groups.bit_length() - 1
    if 1 << steps != groups:
        flow, steps = held(lax.psum(flow, "comm")), 0
    arrived = exchange(0) if steps else None

    rounds = (2 * REACH + 1) * len(TURNS)
    table = degree * block_total
    state = (mine * span, LANES)
    x, *tables, over = pl.pallas_call(
        functools.partial(begin_kernel, mine, degree),
        out_shape=(
            near(state, f32),
            near((rounds * block_total, LANES), i32),
            near((table + rounds * block_total, LANES), f32),
            near((table, LANES), i32),
            near((table, LANES), i32),
            near((table, LANES), f32),
            shape((1,), i32),
        ),
        in_specs=[h(), v()],
        out_specs=(v(), v(), v(), v(), v(), v(), s()),
        scratch_shapes=[
            pltpu.VMEM((mine * block_total, LANES), f32),
            pltpu.VMEM((table, LANES), f32),
            pltpu.SMEM(source_node.shape, i32),
            pltpu.SemaphoreType.DMA((1,)),
        ],
        compiler_params=params,
        name="begin",
    )(far(source_node), received)

    tables = tuple(map(held, tables))
    left = SWEEPS
    for step in range(1, steps):
        flow = pl.pallas_call(
            add_kernel,
            out_shape=near((arc_rows, LANES), f32),
            in_specs=[v(), v()],
            out_specs=v(),
            compiler_params=params,
            name="add",
        )(held(flow), arrived)
        arrived = exchange(step)
        count = min(2 if steps > 2 else 4, left - 2)
        left -= count
        x = pl.pallas_call(
            functools.partial(middle_kernel, mine, degree, count),
            out_shape=near(state, f32),
            in_specs=[s()] + [v()] * (len(tables) + 1),
            out_specs=v(),
            scratch_shapes=[pltpu.VMEM(state, f32)],
            compiler_params=params,
            name="middle",
        )(over, held(x), *tables)

    flows = (held(flow),) if arrived is None else (held(flow), arrived)
    back, gradient = pl.pallas_call(
        functools.partial(end_kernel, mine, degree, left, len(flows)),
        out_shape=(
            near((peers, mine * shard_blocks + SUB, LANES), f32),
            near((degree, shard_nodes), f32),
        ),
        in_specs=[s()] + [v()] * (len(tables) + 2 + len(flows)),
        out_specs=(v(), v()),
        scratch_shapes=[pltpu.VMEM(state, f32), pltpu.VMEM(state, f32)],
        compiler_params=params,
        name="end",
    )(over, held(x), *tables, capacity, *flows)
    final = held(lax.all_to_all(back, "arc", 0, 0, tiled=True))
    return pl.pallas_call(
        functools.partial(final_kernel, mine, degree * node_count),
        out_shape=(shape((commodities, shard_nodes), f32), shape((degree, shard_nodes), f32)),
        in_specs=[v(), v(), v()],
        out_specs=(v(), v()),
        compiler_params=params,
        name="finish",
    )(final, held(gradient), arc_price)


def solution(mesh):
    in_specs = (
        P("comm", "arc"),
        P("comm"),
        P(None, "arc"),
        P(None, "arc"),
        P(None, "arc"),
        P(None, "arc"),
        P(("comm", "arc"), None),
        P(("comm", "arc")),
    )
    out_specs = (P("comm", "arc"), P(None, "arc"))
    return jax.shard_map(shards, mesh=mesh, in_specs=in_specs, out_specs=out_specs, check_vma=False)
```

```python
import functools

import jax
import jax.numpy as jnp
from jax import lax
from jax.experimental import pallas as pl
from jax.experimental.pallas import tpu as pltpu
from jax.sharding import PartitionSpec as P

SWEEPS = 8
REACH = 2
LANES = 128
SUB = 8
VMEM_GRANT = 24 * 1024 * 1024

TURNS = ((None, None), (0, 1), (2, 3), (4, 5), (6, 0))

step_size = 0.25
eps_value = 1e-06


def vmem_spec():
    return pl.BlockSpec(memory_space=pltpu.VMEM)


def smem_spec():
    return pl.BlockSpec(memory_space=pltpu.SMEM)


def three_parts(x):
    first = x.astype(jnp.bfloat16)
    rest = x - first.astype(jnp.float32)
    second = rest.astype(jnp.bfloat16)
    third = (rest - second.astype(jnp.float32)).astype(jnp.bfloat16)
    return first, second, third


def fetch(pairs, sems):
    copies = [pltpu.make_async_copy(src, dst, sems.at[n]) for n, (src, dst) in enumerate(pairs)]
    for copy in copies:
        copy.start()
    return copies


def pack_kernel(
    node_count, path_hbm, demand_hbm, tail_hbm, cost_hbm, price_hbm, dist_hbm, out_ref,
    path_ref, demand_ref, tail_ref, cost_ref, price_ref, dist_ref, sems,
):
    copies = fetch(
        (
            (path_hbm, path_ref),
            (demand_hbm, demand_ref),
            (tail_hbm, tail_ref),
            (cost_hbm, cost_ref),
            (price_hbm, price_ref),
            (dist_hbm, dist_ref),
        ),
        sems,
    )
    peers = out_ref.shape[0]
    degree, shard_nodes = tail_ref.shape
    shard_blocks = shard_nodes // LANES
    mine = dist_ref.shape[0] // peers
    block_total = node_count // LANES
    routes, hops = path_ref.shape

    copies[0].wait()
    copies[1].wait()
    path = path_ref[...]
    slot = path // node_count
    node = path - slot * node_count
    block = node // LANES
    lane = node - block * LANES
    row = block * degree + slot
    row_total = block_total * degree
    row_ids = lax.broadcasted_iota(jnp.int32, (row_total, hops), 0)
    lane_ids = lax.broadcasted_iota(jnp.int32, (LANES, hops), 0)
    left = [[], [], []]
    right = []
    for k in range(routes):
        hit = row_ids == row[k : k + 1, :]
        amount = jnp.full((1, hops), demand_ref[k], jnp.float32)
        for part, piece in enumerate(three_parts(amount)):
            left[part].append(
                jnp.where(hit, piece.astype(jnp.float32), jnp.float32(0.0)).astype(jnp.bfloat16)
            )
        right.append(
            jnp.where(lane_ids == lane[k : k + 1, :], jnp.float32(1.0), jnp.float32(0.0)).astype(
                jnp.bfloat16
            )
        )
    right = jnp.concatenate(right, axis=1)
    flow = None
    for part in (2, 1, 0):
        term = lax.dot_general(
            jnp.concatenate(left[part], axis=1),
            right,
            (((1,), (1,)), ((), ())),
            preferred_element_type=jnp.float32,
        )
        flow = term if flow is None else flow + term

    for copy in copies[2:]:
        copy.wait()
    tail = tail_ref[...].astype(jnp.float32)
    weight = cost_ref[...] + price_ref[...]
    arc_rows = degree * shard_blocks
    base = mine * shard_blocks
    for j in range(peers):
        for b in range(shard_blocks):
            cols = slice(b * LANES, (b + 1) * LANES)
            out_ref[j, b * mine : (b + 1) * mine, :] = dist_ref[j * mine : (j + 1) * mine, cols]
            out_ref[j, base + b * degree : base + (b + 1) * degree, :] = tail[:, cols]
            start = base + arc_rows + b * degree
            out_ref[j, start : start + degree, :] = weight[:, cols]
        start = base + 2 * arc_rows
        out_ref[j, start : start + arc_rows, :] = flow[j * arc_rows : (j + 1) * arc_rows, :]


def halo_store(ref, k, half, groups, span, value):
    blocks = groups * SUB
    base = k * span + SUB
    ref[base + half * SUB : base + (half + 1) * SUB, :] = value
    if half == groups - 1:
        ref[base - REACH : base, :] = value[SUB - REACH :, :]
    if half == 0:
        ref[base + blocks : base + blocks + REACH, :] = value[:REACH, :]


def flow_kernel(rows, buf_ref, flow_ref):
    total = None
    for i in range(buf_ref.shape[0]):
        part = buf_ref[i, buf_ref.shape[1] - rows :, :]
        total = part if total is None else total + part
    flow_ref[...] = total


def plan_rounds(degree, block_total, half, stage, idx_ref, w_ref, left_idx_ref, left_off_ref, left_w_ref):
    groups = block_total // SUB
    width = 2 * REACH + 1
    rows = lax.broadcasted_iota(jnp.int32, (SUB, LANES), 0) + half * SUB
    used = jnp.zeros((SUB, LANES), jnp.int32)
    over = jnp.full((SUB, LANES), degree, jnp.int32)
    lanes_of, weights, bits, opens, offs = [], [], [], [], []
    for s in range(degree):
        at = s * block_total + half * SUB
        tail = stage[at : at + SUB, :].astype(jnp.int32)
        block = tail // LANES
        lane = tail - block * LANES
        off = block - rows + REACH
        off = jnp.where(off < 0, off + block_total, off)
        off = jnp.where(off >= block_total, off - block_total, off)
        weight = w_ref[at : at + SUB, :]
        turned = [jnp.left_shift(1, off)]
        for _ in range(3):
            last = turned[-1]
            turned.append(((last << 1) | (last >> (width - 1))) & (2**width - 1))
        open_rounds = jnp.zeros_like(used)
        for j, (low, high) in enumerate(TURNS):
            if low is None:
                spot = turned[0]
            else:
                by_low = ((lane >> low) & 1) == 1
                by_high = ((lane >> high) & 1) == 1
                spot = jnp.where(
                    by_high,
                    jnp.where(by_low, turned[3], turned[2]),
                    jnp.where(by_low, turned[1], turned[0]),
                )
            open_rounds = open_rounds | (spot << (width * j))
        free = open_rounds & ~used
        bit = free & -free
        if s >= len(TURNS):
            movable = jnp.zeros_like(used)
            targets = []
            for earlier, taken in zip(opens, bits):
                target = earlier & ~used
                targets.append(target)
                movable = movable | jnp.where(target != 0, taken, 0)
            wanted = open_rounds & movable
            wanted = jnp.where(bit == 0, wanted & -wanted, 0)
            for e, (target, taken) in enumerate(zip(targets, bits)):
                moved = (taken & wanted) != 0
                target = jnp.where(moved, target & -target, 0)
                used = used | target
                bits[e] = jnp.where(moved, target, taken)
            bit = bit | wanted
        used = used | bit
        over = jnp.minimum(over, jnp.where(bit == 0, s, degree))
        opens.append(open_rounds)
        offs.append(off)
        lanes_of.append(lane)
        weights.append(weight)
        bits.append(bit)
    for s in range(degree):
        at = s * block_total + half * SUB
        left_idx_ref[at : at + SUB, :] = lanes_of[s]
        left_off_ref[at : at + SUB, :] = offs[s]
        left_w_ref[at : at + SUB, :] = jnp.where(bits[s] == 0, weights[s], jnp.float32(jnp.inf))
    for r in range(width * len(TURNS)):
        idx = jnp.zeros((SUB, LANES), jnp.int32)
        weight = jnp.full((SUB, LANES), jnp.inf, jnp.float32)
        for s in range(degree):
            hit = bits[s] == (1 << r)
            idx = jnp.where(hit, lanes_of[s], idx)
            weight = jnp.where(hit, weights[s], weight)
        at = (r * groups + half) * SUB
        idx_ref[at : at + SUB, :] = idx
        w_ref[degree * block_total + at : degree * block_total + at + SUB, :] = weight
    return over


def sweep_once(mine, degree, first_over, src, dst, tables):
    idx_ref, w_ref, left_idx_ref, left_off_ref, left_w_ref = tables
    span = src.shape[0] // mine
    block_total = span - 2 * SUB
    groups = block_total // SUB
    width = 2 * REACH + 1
    w_base = degree * block_total
    lane = lax.broadcasted_iota(jnp.int32, (SUB, LANES), 1)
    bit_masks = [((lane >> t) & 1) == 1 for t in range(LANES.bit_length() - 1)]
    for half in range(groups):
        best = [src[k * span + SUB + half * SUB : k * span + SUB + (half + 1) * SUB, :] for k in range(mine)]
        for j, (low, high) in enumerate(TURNS):
            for q in range(width):
                at = ((j * width + q) * groups + half) * SUB
                idx = idx_ref[at : at + SUB, :]
                w = w_ref[w_base + at : w_base + at + SUB, :]
                for k in range(mine):
                    base = k * span + SUB + half * SUB - REACH

                    def block(turned):
                        o = base + (q - turned) % width
                        return src[o : o + SUB, :]

                    if low is None:
                        shown = block(0)
                    else:
                        shown = jnp.where(
                            bit_masks[high],
                            jnp.where(bit_masks[low], block(3), block(2)),
                            jnp.where(bit_masks[low], block(1), block(0)),
                        )
                    value = jnp.take_along_axis(shown, idx, axis=1, mode="promise_in_bounds")
                    best[k] = jnp.minimum(best[k], value + w)
        for k in range(mine):
            halo_store(dst, k, half, groups, span, best[k])

    @pl.loop(first_over, degree)
    def _(s):
        for half in range(groups):
            at = pl.multiple_of(s * block_total + half * SUB, SUB)
            idx = left_idx_ref[pl.ds(at, SUB), :]
            off = left_off_ref[pl.ds(at, SUB), :]
            w = left_w_ref[pl.ds(at, SUB), :]
            for k in range(mine):
                base = k * span + SUB + half * SUB
                picked = None
                for o in range(width):
                    start = base + o - REACH
                    value = jnp.take_along_axis(
                        src[start : start + SUB, :], idx, axis=1, mode="promise_in_bounds"
                    )
                    picked = value if picked is None else jnp.where(off == o, value, picked)
                now = dst[base : base + SUB, :]
                halo_store(dst, k, half, groups, span, jnp.minimum(now, picked + w))


def sweep_pairs(count, mine, degree, first_over, one, two, tables):
    @pl.loop(0, count // 2)
    def _(_):
        sweep_once(mine, degree, first_over, one, two, tables)
        sweep_once(mine, degree, first_over, two, one, tables)


def begin_kernel(
    mine, degree, source_hbm, buf_ref,
    x_ref, idx_ref, w_ref, left_idx_ref, left_off_ref, left_w_ref, over_ref,
    stage, stage_tail, source_ref, sems,
):
    (copy,) = fetch(((source_hbm, source_ref),), sems)
    peers = buf_ref.shape[0]
    span = x_ref.shape[0] // mine
    block_total = span - 2 * SUB
    groups = block_total // SUB
    shard_blocks = block_total // peers
    arc_rows = degree * shard_blocks
    base = mine * shard_blocks
    for i in range(peers):
        for b in range(shard_blocks):
            blk = i * shard_blocks + b
            stage[pl.ds(blk, mine, stride=block_total), :] = buf_ref[i, b * mine : (b + 1) * mine, :]
            s0 = base + b * degree
            stage_tail[pl.ds(blk, degree, stride=block_total), :] = buf_ref[i, s0 : s0 + degree, :]
            s1 = base + arc_rows + b * degree
            w_ref[pl.ds(blk, degree, stride=block_total), :] = buf_ref[i, s1 : s1 + degree, :]
    over = None
    for half in range(groups):
        part = plan_rounds(
            degree, block_total, half, stage_tail, idx_ref, w_ref,
            left_idx_ref, left_off_ref, left_w_ref,
        )
        over = part if over is None else jnp.minimum(over, part)
    over_ref[0] = jnp.min(over.astype(jnp.float32)).astype(jnp.int32)
    copy.wait()
    rows = lax.broadcasted_iota(jnp.int32, (SUB, LANES), 0)
    lanes = lax.broadcasted_iota(jnp.int32, (SUB, LANES), 1)
    first = lax.axis_index("arc") * mine
    for half in range(groups):
        node = (rows + half * SUB) * LANES + lanes
        for k in range(mine):
            at = k * block_total + half * SUB
            value = jnp.where(node == source_ref[first + k], jnp.float32(0.0), stage[at : at + SUB, :])
            halo_store(x_ref, k, half, groups, span, value)


def add_kernel(a_ref, b_ref, after_ref, out_ref):
    out_ref[...] = a_ref[...] + b_ref[...]


def middle_kernel(
    mine, degree, count, over_ref, start_ref, idx_ref, w_ref, left_idx_ref, left_off_ref,
    left_w_ref, x_ref, other,
):
    x_ref[...] = start_ref[...]
    tables = (idx_ref, w_ref, left_idx_ref, left_off_ref, left_w_ref)
    sweep_pairs(count, mine, degree, over_ref[0], x_ref, other, tables)


def end_kernel(
    mine, degree, count, parts, over_ref, start_ref, idx_ref, w_ref, left_idx_ref, left_off_ref,
    left_w_ref, cap_ref, *refs,
):
    flow_refs, (out_ref, grad_ref, x_ref, other) = refs[:parts], refs[parts:]
    peers = out_ref.shape[0]
    span = x_ref.shape[0] // mine
    block_total = span - 2 * SUB
    shard_blocks = block_total // peers
    tables = (idx_ref, w_ref, left_idx_ref, left_off_ref, left_w_ref)
    first_over = over_ref[0]
    x_ref[...] = start_ref[...]
    sweep_pairs(count, mine, degree, first_over, x_ref, other, tables)
    square = None
    for b in range(shard_blocks):
        cols = slice(b * LANES, (b + 1) * LANES)
        flow = None
        for ref in flow_refs:
            part = ref[b * degree : (b + 1) * degree, :]
            flow = part if flow is None else flow + part
        grad = flow - cap_ref[:, cols]
        grad_ref[:, cols] = grad
        term = grad * grad
        square = term if square is None else square + term
    folded = jnp.sum(square.reshape(degree // SUB, SUB, LANES), axis=0)
    base = mine * shard_blocks
    for i in range(peers):
        for b in range(shard_blocks):
            blk = SUB + i * shard_blocks + b
            out_ref[i, b * mine : (b + 1) * mine, :] = x_ref[pl.ds(blk, mine, stride=span), :]
        out_ref[i, base : base + SUB, :] = folded


def final_kernel(mine, arc_total, buf_ref, grad_ref, price_ref, dist_ref, new_ref):
    peers = buf_ref.shape[0]
    shard_blocks = dist_ref.shape[1] // LANES
    base = mine * shard_blocks
    total = None
    for i in range(peers):
        for b in range(shard_blocks):
            dist_ref[i * mine : (i + 1) * mine, b * LANES : (b + 1) * LANES] = buf_ref[
                i, b * mine : (b + 1) * mine, :
            ]
        part = buf_ref[i, base : base + SUB, :]
        total = part if total is None else total + part
    square_sum = jnp.sum(jnp.sum(total, axis=1, keepdims=True), axis=0, keepdims=True)
    scale_root = jnp.sqrt(square_sum / arc_total + eps_value)
    new_ref[...] = jnp.maximum(
        price_ref[...] + step_size * grad_ref[...] / scale_root, jnp.float32(0.0)
    )


def shards(prev_dist, source_node, arc_tail, base_cost, arc_price, capacity, path_arcs, demand):
    commodities, shard_nodes = prev_dist.shape
    peers = lax.axis_size("arc")
    groups = lax.axis_size("comm")
    node_count = shard_nodes * peers
    degree = arc_tail.shape[0]
    mine = commodities // peers
    shard_blocks = shard_nodes // LANES
    block_total = node_count // LANES
    span = block_total + 2 * SUB
    arc_rows = degree * shard_blocks
    f32, i32 = jnp.float32, jnp.int32
    shape = jax.ShapeDtypeStruct
    near = pltpu.VMEM
    v, s = vmem_spec, smem_spec

    def held(x):
        return pltpu.with_memory_space_constraint(x, pltpu.VMEM)

    def far(x):
        return pltpu.with_memory_space_constraint(x, pltpu.HBM)

    def scratch(*arrays):
        return [pltpu.VMEM(x.shape, x.dtype) for x in arrays]

    h = functools.partial(pl.BlockSpec, memory_space=pltpu.HBM)
    params = pltpu.CompilerParams(vmem_limit_bytes=VMEM_GRANT)
    arcs = (arc_tail, base_cost, arc_price, prev_dist)
    packed = pl.pallas_call(
        functools.partial(pack_kernel, node_count),
        out_shape=near((peers, mine * shard_blocks + 3 * arc_rows, LANES), f32),
        in_specs=[h()] * 6,
        out_specs=v(),
        scratch_shapes=[
            *scratch(path_arcs),
            pltpu.SMEM(demand.shape, f32),
            *scratch(*arcs),
            pltpu.SemaphoreType.DMA((6,)),
        ],
        compiler_params=params,
        name="pack",
    )(far(path_arcs), far(demand), *map(far, arcs))
    received = held(lax.all_to_all(packed, "arc", 0, 0, tiled=True))

    flow = pl.pallas_call(
        functools.partial(flow_kernel, arc_rows),
        out_shape=near((arc_rows, LANES), f32),
        in_specs=[v()],
        out_specs=v(),
        compiler_params=params,
        name="flow",
    )(received)

    def exchange(step):
        pairs = [(i, i ^ (1 << step)) for i in range(groups)]
        return held(lax.ppermute(flow, "comm", pairs))

    steps = groups.bit_length() - 1
    if 1 << steps != groups:
        flow, steps = held(lax.psum(flow, "comm")), 0
    arrived = exchange(0) if steps else None

    rounds = (2 * REACH + 1) * len(TURNS)
    table = degree * block_total
    state = (mine * span, LANES)
    x, *tables, over = pl.pallas_call(
        functools.partial(begin_kernel, mine, degree),
        out_shape=(
            near(state, f32),
            near((rounds * block_total, LANES), i32),
            near((table + rounds * block_total, LANES), f32),
            near((table, LANES), i32),
            near((table, LANES), i32),
            near((table, LANES), f32),
            shape((1,), i32),
        ),
        in_specs=[h(), v()],
        out_specs=(v(), v(), v(), v(), v(), v(), s()),
        scratch_shapes=[
            pltpu.VMEM((mine * block_total, LANES), f32),
            pltpu.VMEM((table, LANES), f32),
            pltpu.SMEM(source_node.shape, i32),
            pltpu.SemaphoreType.DMA((1,)),
        ],
        compiler_params=params,
        name="begin",
    )(far(source_node), received)

    tables = tuple(map(held, tables))
    left = SWEEPS
    for step in range(1, steps):
        flow = pl.pallas_call(
            add_kernel,
            out_shape=near((arc_rows, LANES), f32),
            in_specs=[v(), v(), v()],
            out_specs=v(),
            compiler_params=params,
            name="add",
        )(held(flow), arrived, held(x))
        arrived = exchange(step)
        count = min(2 if steps > 2 else 4, left - 2)
        left -= count
        x = pl.pallas_call(
            functools.partial(middle_kernel, mine, degree, count),
            out_shape=near(state, f32),
            in_specs=[s()] + [v()] * (len(tables) + 1),
            out_specs=v(),
            scratch_shapes=[pltpu.VMEM(state, f32)],
            compiler_params=params,
                name="middle",
        )(over, held(x), *tables)

    flows = (held(flow),) if arrived is None else (held(flow), arrived)
    back, gradient = pl.pallas_call(
        functools.partial(end_kernel, mine, degree, left, len(flows)),
        out_shape=(
            near((peers, mine * shard_blocks + SUB, LANES), f32),
            near((degree, shard_nodes), f32),
        ),
        in_specs=[s()] + [v()] * (len(tables) + 2 + len(flows)),
        out_specs=(v(), v()),
        scratch_shapes=[pltpu.VMEM(state, f32), pltpu.VMEM(state, f32)],
        compiler_params=params,
        name="end",
    )(over, held(x), *tables, capacity, *flows)
    final = held(lax.all_to_all(back, "arc", 0, 0, tiled=True))
    return pl.pallas_call(
        functools.partial(final_kernel, mine, degree * node_count),
        out_shape=(shape((commodities, shard_nodes), f32), shape((degree, shard_nodes), f32)),
        in_specs=[v(), v(), v()],
        out_specs=(v(), v()),
        compiler_params=params,
        name="finish",
    )(final, held(gradient), arc_price)


def solution(mesh):
    in_specs = (
        P("comm", "arc"),
        P("comm"),
        P(None, "arc"),
        P(None, "arc"),
        P(None, "arc"),
        P(None, "arc"),
        P(("comm", "arc"), None),
        P(("comm", "arc")),
    )
    out_specs = (P("comm", "arc"), P(None, "arc"))
    return jax.shard_map(shards, mesh=mesh, in_specs=in_specs, out_specs=out_specs, check_vma=False)
```

```python
import functools

import jax
import jax.numpy as jnp
from jax import lax
from jax.experimental import pallas as pl
from jax.experimental.pallas import tpu as pltpu
from jax.sharding import PartitionSpec as P

SWEEPS = 8
REACH = 2
LANES = 128
SUB = 8
PAD = 2 * REACH + 1
VMEM_GRANT = 24 * 1024 * 1024

TURNS = ((None, None, 5), (0, 1, 5), (2, 3, 5), (4, 5, 5), (6, 0, 2))
ROUNDS = sum(turn[2] for turn in TURNS)

step_size = 0.25
eps_value = 1e-06


def vmem_spec():
    return pl.BlockSpec(memory_space=pltpu.VMEM)


def three_parts(x):
    first = x.astype(jnp.bfloat16)
    rest = x - first.astype(jnp.float32)
    second = rest.astype(jnp.bfloat16)
    third = (rest - second.astype(jnp.float32)).astype(jnp.bfloat16)
    return first, second, third


def fetch(pairs, sems):
    copies = [pltpu.make_async_copy(src, dst, sems.at[n]) for n, (src, dst) in enumerate(pairs)]
    for copy in copies:
        copy.start()
    return copies


def pack_kernel(
    node_count, path_hbm, demand_hbm, tail_hbm, cost_hbm, price_hbm, dist_hbm, out_ref,
    path_ref, demand_ref, tail_ref, cost_ref, price_ref, dist_ref, sems,
):
    copies = fetch(
        (
            (path_hbm, path_ref),
            (demand_hbm, demand_ref),
            (tail_hbm, tail_ref),
            (cost_hbm, cost_ref),
            (price_hbm, price_ref),
            (dist_hbm, dist_ref),
        ),
        sems,
    )
    peers = out_ref.shape[0]
    degree, shard_nodes = tail_ref.shape
    shard_blocks = shard_nodes // LANES
    mine = dist_ref.shape[0] // peers
    block_total = node_count // LANES
    routes, hops = path_ref.shape

    copies[0].wait()
    copies[1].wait()
    path = path_ref[...]
    slot = path // node_count
    node = path - slot * node_count
    block = node // LANES
    lane = node - block * LANES
    row = block * degree + slot
    row_total = block_total * degree
    row_ids = lax.broadcasted_iota(jnp.int32, (row_total, hops), 0)
    lane_ids = lax.broadcasted_iota(jnp.int32, (LANES, hops), 0)
    left = [[], [], []]
    right = []
    for k in range(routes):
        hit = row_ids == row[k : k + 1, :]
        amount = jnp.full((1, hops), demand_ref[k], jnp.float32)
        for part, piece in enumerate(three_parts(amount)):
            left[part].append(
                jnp.where(hit, piece.astype(jnp.float32), jnp.float32(0.0)).astype(jnp.bfloat16)
            )
        right.append(
            jnp.where(lane_ids == lane[k : k + 1, :], jnp.float32(1.0), jnp.float32(0.0)).astype(
                jnp.bfloat16
            )
        )
    right = jnp.concatenate(right, axis=1)
    flow = None
    for part in (2, 1, 0):
        term = lax.dot_general(
            jnp.concatenate(left[part], axis=1),
            right,
            (((1,), (1,)), ((), ())),
            preferred_element_type=jnp.float32,
        )
        flow = term if flow is None else flow + term

    for copy in copies[2:]:
        copy.wait()
    tail = tail_ref[...].astype(jnp.float32)
    weight = cost_ref[...] + price_ref[...]
    arc_rows = degree * shard_blocks
    base = mine * shard_blocks
    for j in range(peers):
        for b in range(shard_blocks):
            cols = slice(b * LANES, (b + 1) * LANES)
            out_ref[j, b * mine : (b + 1) * mine, :] = dist_ref[j * mine : (j + 1) * mine, cols]
            out_ref[j, base + b * degree : base + (b + 1) * degree, :] = tail[:, cols]
            start = base + arc_rows + b * degree
            out_ref[j, start : start + degree, :] = weight[:, cols]
        start = base + 2 * arc_rows
        out_ref[j, start : start + arc_rows, :] = flow[j * arc_rows : (j + 1) * arc_rows, :]


def halo_store(ref, k, half, groups, span, value):
    blocks = groups * SUB
    base = k * span + REACH
    ref[base + half * SUB : base + (half + 1) * SUB, :] = value
    if half == groups - 1:
        ref[base - REACH : base, :] = value[SUB - REACH :, :]
    if half == 0:
        ref[base + blocks : base + blocks + REACH, :] = value[:REACH, :]


def flow_kernel(rows, buf_ref, flow_ref):
    total = None
    for i in range(buf_ref.shape[0]):
        part = buf_ref[i, buf_ref.shape[1] - rows :, :]
        total = part if total is None else total + part
    flow_ref[...] = total


def plan_rounds(
    degree, block_total, half, stage, stage_w, idx_ref, w_ref, left_idx_ref, left_off_ref, left_w_ref
):
    groups = block_total // SUB
    width = 2 * REACH + 1
    rows = lax.broadcasted_iota(jnp.int32, (SUB, LANES), 0) + half * SUB
    used = jnp.zeros((SUB, LANES), jnp.int32)
    over = jnp.full((SUB, LANES), degree, jnp.int32)
    lanes_of, weights, bits, opens, offs = [], [], [], [], []
    for s in range(degree):
        at = s * (stage.shape[0] // degree) + half * SUB
        tail = stage[at : at + SUB, :].astype(jnp.int32)
        block = tail // LANES
        lane = tail - block * LANES
        off = block - rows + REACH
        off = jnp.where(off < 0, off + block_total, off)
        off = jnp.where(off >= block_total, off - block_total, off)
        weight = stage_w[at : at + SUB, :]
        turned = [jnp.left_shift(1, off)]
        for _ in range(3):
            last = turned[-1]
            turned.append(((last << 1) | (last >> (width - 1))) & (2**width - 1))
        open_rounds = jnp.zeros_like(used)
        for j, (low, high, count) in enumerate(TURNS):
            if low is None:
                spot = turned[0]
            else:
                by_low = ((lane >> low) & 1) == 1
                by_high = ((lane >> high) & 1) == 1
                spot = jnp.where(
                    by_high,
                    jnp.where(by_low, turned[3], turned[2]),
                    jnp.where(by_low, turned[1], turned[0]),
                )
            if count < width:
                spot = spot & (2**count - 1)
            open_rounds = open_rounds | (spot << (width * j))
        free = open_rounds & ~used
        bit = free & -free
        if s >= len(TURNS) - 1:
            near, far = jnp.zeros_like(used), jnp.zeros_like(used)
            for earlier, taken in zip(opens, bits):
                near = near | jnp.where((earlier & ~used) != 0, taken, 0)
            for earlier, taken in zip(opens, bits):
                far = far | jnp.where((earlier & near) != 0, taken, 0)
            straight = open_rounds & near
            wanted = jnp.where(straight != 0, straight, open_rounds & far)
            wanted = jnp.where(bit == 0, wanted & -wanted, 0)
            twice = jnp.where(straight != 0, 0, wanted)
            passed = jnp.zeros_like(used)
            chain = []
            for earlier, taken in zip(opens, bits):
                target = earlier & near
                target = jnp.where((taken & twice) != 0, target & -target, 0)
                passed = passed | target
                chain.append(target)
            last = jnp.where(straight != 0, wanted, passed)
            freed = ~used
            for e, (earlier, taken, target) in enumerate(zip(opens, bits, chain)):
                end = earlier & freed
                end = jnp.where((taken & last) != 0, end & -end, 0)
                used = used | end
                moved = target | end
                bits[e] = jnp.where(moved != 0, moved, taken)
            bit = bit | wanted
        used = used | bit
        over = jnp.minimum(over, jnp.where(bit == 0, s, degree))
        opens.append(open_rounds)
        offs.append(off)
        lanes_of.append(lane)
        weights.append(weight)
        bits.append(bit)
    for s in range(degree):
        at = s * block_total + half * SUB
        left_idx_ref[at : at + SUB, :] = lanes_of[s]
        left_off_ref[at : at + SUB, :] = offs[s]
        left_w_ref[at : at + SUB, :] = jnp.where(bits[s] == 0, weights[s], jnp.float32(jnp.inf))
    for r in range(ROUNDS):
        idx = jnp.zeros((SUB, LANES), jnp.int32)
        weight = jnp.full((SUB, LANES), jnp.inf, jnp.float32)
        for s in range(degree):
            hit = bits[s] == (1 << r)
            idx = jnp.where(hit, lanes_of[s], idx)
            weight = jnp.where(hit, weights[s], weight)
        at = (r * groups + half) * SUB
        idx_ref[at : at + SUB, :] = idx
        w_ref[at : at + SUB, :] = weight
    return over


def sweep_once(mine, degree, first_over, src, dst, tables):
    idx_ref, w_ref, left_idx_ref, left_off_ref, left_w_ref = tables
    span = src.shape[0] // mine
    block_total = span - PAD
    groups = block_total // SUB
    width = 2 * REACH + 1
    lane = lax.broadcasted_iota(jnp.int32, (SUB, LANES), 1)
    bit_masks = [((lane >> t) & 1) == 1 for t in range(LANES.bit_length() - 1)]
    for half in range(groups):
        best = [src[k * span + REACH + half * SUB : k * span + REACH + (half + 1) * SUB, :] for k in range(mine)]
        for j, (low, high, count) in enumerate(TURNS):
            for q in range(count):
                at = ((j * width + q) * groups + half) * SUB
                idx = idx_ref[at : at + SUB, :]
                w = w_ref[at : at + SUB, :]
                for k in range(mine):
                    base = k * span + half * SUB

                    def block(turned):
                        o = base + (q - turned) % width
                        return src[o : o + SUB, :]

                    if low is None:
                        shown = block(0)
                    else:
                        shown = jnp.where(
                            bit_masks[high],
                            jnp.where(bit_masks[low], block(3), block(2)),
                            jnp.where(bit_masks[low], block(1), block(0)),
                        )
                    value = jnp.take_along_axis(shown, idx, axis=1, mode="promise_in_bounds")
                    best[k] = jnp.minimum(best[k], value + w)
        for k in range(mine):
            halo_store(dst, k, half, groups, span, best[k])

    @pl.loop(first_over, degree)
    def _(s):
        for half in range(groups):
            at = pl.multiple_of(s * block_total + half * SUB, SUB)
            idx = left_idx_ref[pl.ds(at, SUB), :]
            off = left_off_ref[pl.ds(at, SUB), :]
            w = left_w_ref[pl.ds(at, SUB), :]
            for k in range(mine):
                base = k * span + REACH + half * SUB
                picked = None
                for o in range(width):
                    start = base + o - REACH
                    value = jnp.take_along_axis(
                        src[start : start + SUB, :], idx, axis=1, mode="promise_in_bounds"
                    )
                    picked = value if picked is None else jnp.where(off == o, value, picked)
                now = dst[base : base + SUB, :]
                halo_store(dst, k, half, groups, span, jnp.minimum(now, picked + w))


def sweep_pairs(count, mine, degree, first_over, one, two, tables):
    @pl.loop(0, count // 2)
    def _(_):
        sweep_once(mine, degree, first_over, one, two, tables)
        sweep_once(mine, degree, first_over, two, one, tables)


def begin_kernel(
    mine, degree, source_hbm, buf_ref,
    x_ref, idx_ref, w_ref, left_idx_ref, left_off_ref, left_w_ref, over_ref,
    stage, stage_tail, stage_w, source_ref, sems,
):
    (copy,) = fetch(((source_hbm, source_ref),), sems)
    pitch = stage.shape[0] // mine
    peers = buf_ref.shape[0]
    span = x_ref.shape[0] // mine
    block_total = span - PAD
    groups = block_total // SUB
    shard_blocks = block_total // peers
    arc_rows = degree * shard_blocks
    base = mine * shard_blocks
    for i in range(peers):
        for b in range(shard_blocks):
            blk = i * shard_blocks + b
            stage[pl.ds(blk, mine, stride=pitch), :] = buf_ref[i, b * mine : (b + 1) * mine, :]
            s0 = base + b * degree
            stage_tail[pl.ds(blk, degree, stride=pitch), :] = buf_ref[i, s0 : s0 + degree, :]
            s1 = base + arc_rows + b * degree
            stage_w[pl.ds(blk, degree, stride=pitch), :] = buf_ref[i, s1 : s1 + degree, :]
    over = None
    for half in range(groups):
        part = plan_rounds(
            degree, block_total, half, stage_tail, stage_w, idx_ref, w_ref,
            left_idx_ref, left_off_ref, left_w_ref,
        )
        over = part if over is None else jnp.minimum(over, part)
    copy.wait()
    rows = lax.broadcasted_iota(jnp.int32, (SUB, LANES), 0)
    lanes = lax.broadcasted_iota(jnp.int32, (SUB, LANES), 1)
    first = lax.axis_index("arc") * mine
    for half in range(groups):
        node = (rows + half * SUB) * LANES + lanes
        for k in range(mine):
            at = k * pitch + half * SUB
            value = jnp.where(node == source_ref[first + k], jnp.float32(0.0), stage[at : at + SUB, :])
            halo_store(x_ref, k, half, groups, span, value)
    over_ref[...] = jnp.full(over_ref.shape, jnp.min(over.astype(jnp.float32)).astype(jnp.int32))


def add_kernel(a_ref, b_ref, after_ref, out_ref):
    out_ref[...] = a_ref[...] + b_ref[...]


def middle_kernel(
    mine, degree, count, over_ref, start_ref, idx_ref, w_ref, left_idx_ref, left_off_ref,
    left_w_ref, x_ref, other,
):
    x_ref[...] = start_ref[...]
    tables = (idx_ref, w_ref, left_idx_ref, left_off_ref, left_w_ref)
    sweep_pairs(count, mine, degree, over_ref[0, 0], x_ref, other, tables)


def end_kernel(
    mine, degree, count, parts, over_ref, start_ref, idx_ref, w_ref, left_idx_ref, left_off_ref,
    left_w_ref, cap_ref, *refs,
):
    flow_refs, (out_ref, grad_ref, x_ref, other) = refs[:parts], refs[parts:]
    peers = out_ref.shape[0]
    span = x_ref.shape[0] // mine
    block_total = span - PAD
    shard_blocks = block_total // peers
    tables = (idx_ref, w_ref, left_idx_ref, left_off_ref, left_w_ref)
    first_over = over_ref[0, 0]
    x_ref[...] = start_ref[...]
    sweep_pairs(count, mine, degree, first_over, x_ref, other, tables)
    square = None
    for b in range(shard_blocks):
        cols = slice(b * LANES, (b + 1) * LANES)
        flow = None
        for ref in flow_refs:
            part = ref[b * degree : (b + 1) * degree, :]
            flow = part if flow is None else flow + part
        grad = flow - cap_ref[:, cols]
        grad_ref[:, cols] = grad
        term = grad * grad
        square = term if square is None else square + term
    folded = jnp.sum(square.reshape(degree // SUB, SUB, LANES), axis=0)
    base = mine * shard_blocks
    for i in range(peers):
        for b in range(shard_blocks):
            blk = REACH + i * shard_blocks + b
            out_ref[i, b * mine : (b + 1) * mine, :] = x_ref[pl.ds(blk, mine, stride=span), :]
        out_ref[i, base : base + SUB, :] = folded


def final_kernel(mine, arc_total, buf_ref, grad_ref, price_ref, dist_ref, new_ref):
    peers = buf_ref.shape[0]
    shard_blocks = dist_ref.shape[1] // LANES
    base = mine * shard_blocks
    total = None
    for i in range(peers):
        for b in range(shard_blocks):
            dist_ref[i * mine : (i + 1) * mine, b * LANES : (b + 1) * LANES] = buf_ref[
                i, b * mine : (b + 1) * mine, :
            ]
        part = buf_ref[i, base : base + SUB, :]
        total = part if total is None else total + part
    square_sum = jnp.sum(jnp.sum(total, axis=1, keepdims=True), axis=0, keepdims=True)
    scale_root = jnp.sqrt(square_sum / arc_total + eps_value)
    new_ref[...] = jnp.maximum(
        price_ref[...] + step_size * grad_ref[...] / scale_root, jnp.float32(0.0)
    )


def shards(prev_dist, source_node, arc_tail, base_cost, arc_price, capacity, path_arcs, demand):
    commodities, shard_nodes = prev_dist.shape
    peers = lax.axis_size("arc")
    groups = lax.axis_size("comm")
    node_count = shard_nodes * peers
    degree = arc_tail.shape[0]
    mine = commodities // peers
    shard_blocks = shard_nodes // LANES
    block_total = node_count // LANES
    span = block_total + PAD
    arc_rows = degree * shard_blocks
    f32, i32 = jnp.float32, jnp.int32
    shape = jax.ShapeDtypeStruct
    near = pltpu.VMEM
    v = vmem_spec

    def held(x):
        return pltpu.with_memory_space_constraint(x, pltpu.VMEM)

    def far(x):
        return pltpu.with_memory_space_constraint(x, pltpu.HBM)

    def scratch(*arrays):
        return [pltpu.VMEM(x.shape, x.dtype) for x in arrays]

    h = functools.partial(pl.BlockSpec, memory_space=pltpu.HBM)
    params = pltpu.CompilerParams(vmem_limit_bytes=VMEM_GRANT)
    arcs = (arc_tail, base_cost, arc_price, prev_dist)
    packed = pl.pallas_call(
        functools.partial(pack_kernel, node_count),
        out_shape=near((peers, mine * shard_blocks + 3 * arc_rows, LANES), f32),
        in_specs=[h()] * 6,
        out_specs=v(),
        scratch_shapes=[
            *scratch(path_arcs),
            pltpu.SMEM(demand.shape, f32),
            *scratch(*arcs),
            pltpu.SemaphoreType.DMA((6,)),
        ],
        compiler_params=params,
        name="pack",
    )(far(path_arcs), far(demand), *map(far, arcs))
    received = held(lax.all_to_all(packed, "arc", 0, 0, tiled=True))

    flow = pl.pallas_call(
        functools.partial(flow_kernel, arc_rows),
        out_shape=near((arc_rows, LANES), f32),
        in_specs=[v()],
        out_specs=v(),
        compiler_params=params,
        name="flow",
    )(received)

    def exchange(step):
        pairs = [(i, i ^ (1 << step)) for i in range(groups)]
        return held(lax.ppermute(flow, "comm", pairs))

    steps = groups.bit_length() - 1
    if 1 << steps != groups:
        flow, steps = held(lax.psum(flow, "comm")), 0
    arrived = exchange(0) if steps else None

    rounds = ROUNDS
    table = degree * block_total
    state = (mine * span, LANES)
    x, *tables, over = pl.pallas_call(
        functools.partial(begin_kernel, mine, degree),
        out_shape=(
            near(state, f32),
            near((rounds * block_total, LANES), i32),
            near((rounds * block_total, LANES), f32),
            near((table, LANES), i32),
            near((table, LANES), i32),
            near((table, LANES), f32),
            near((SUB, LANES), i32),
        ),
        in_specs=[h(), v()],
        out_specs=(v(),) * 7,
        scratch_shapes=[
            pltpu.VMEM((mine * (block_total + 1), LANES), f32),
            pltpu.VMEM((degree * (block_total + 1), LANES), f32),
            pltpu.VMEM((degree * (block_total + 1), LANES), f32),
            pltpu.SMEM(source_node.shape, i32),
            pltpu.SemaphoreType.DMA((1,)),
        ],
        compiler_params=params,
        name="begin",
    )(far(source_node), received)

    tables, over = tuple(map(held, tables)), held(over)
    left = SWEEPS
    for step in range(1, steps):
        flow = pl.pallas_call(
            add_kernel,
            out_shape=near((arc_rows, LANES), f32),
            in_specs=[v(), v(), v()],
            out_specs=v(),
            compiler_params=params,
            name="add",
        )(held(flow), arrived, held(x))
        arrived = exchange(step)
        count = min(2 if steps > 2 else 4, left - 2)
        left -= count
        x = pl.pallas_call(
            functools.partial(middle_kernel, mine, degree, count),
            out_shape=near(state, f32),
            in_specs=[v()] * (len(tables) + 2),
            out_specs=v(),
            scratch_shapes=[pltpu.VMEM(state, f32)],
            compiler_params=params,
                name="middle",
        )(over, held(x), *tables)

    flows = (held(flow),) if arrived is None else (held(flow), arrived)
    back, gradient = pl.pallas_call(
        functools.partial(end_kernel, mine, degree, left, len(flows)),
        out_shape=(
            near((peers, mine * shard_blocks + SUB, LANES), f32),
            near((degree, shard_nodes), f32),
        ),
        in_specs=[v()] * (len(tables) + 3 + len(flows)),
        out_specs=(v(), v()),
        scratch_shapes=[pltpu.VMEM(state, f32), pltpu.VMEM(state, f32)],
        compiler_params=params,
        name="end",
    )(over, held(x), *tables, capacity, *flows)
    final = held(lax.all_to_all(back, "arc", 0, 0, tiled=True))
    return pl.pallas_call(
        functools.partial(final_kernel, mine, degree * node_count),
        out_shape=(shape((commodities, shard_nodes), f32), shape((degree, shard_nodes), f32)),
        in_specs=[v(), v(), v()],
        out_specs=(v(), v()),
        compiler_params=params,
        name="finish",
    )(final, held(gradient), arc_price)


def solution(mesh):
    in_specs = (
        P("comm", "arc"),
        P("comm"),
        P(None, "arc"),
        P(None, "arc"),
        P(None, "arc"),
        P(None, "arc"),
        P(("comm", "arc"), None),
        P(("comm", "arc")),
    )
    out_specs = (P("comm", "arc"), P(None, "arc"))
    return jax.shard_map(shards, mesh=mesh, in_specs=in_specs, out_specs=out_specs, check_vma=False)
```

```python
import functools

import jax
import jax.numpy as jnp
from jax import lax
from jax.experimental import pallas as pl
from jax.experimental.pallas import tpu as pltpu
from jax.sharding import PartitionSpec as P

SWEEPS = 8
REACH = 2
LANES = 128
SUB = 8
PAD = 2 * REACH + 1
VMEM_GRANT = 24 * 1024 * 1024

TURNS = ((None, None, 5), (0, 1, 5), (2, 3, 5), (4, 5, 5), (6, 0, 2))
ROUNDS = sum(turn[2] for turn in TURNS)

step_size = 0.25
eps_value = 1e-06


def vmem_spec():
    return pl.BlockSpec(memory_space=pltpu.VMEM)


def three_parts(x):
    first = x.astype(jnp.bfloat16)
    rest = x - first.astype(jnp.float32)
    second = rest.astype(jnp.bfloat16)
    third = (rest - second.astype(jnp.float32)).astype(jnp.bfloat16)
    return first, second, third


def fetch(pairs, sems):
    copies = [pltpu.make_async_copy(src, dst, sems.at[n]) for n, (src, dst) in enumerate(pairs)]
    for copy in copies:
        copy.start()
    return copies


def pack_kernel(
    node_count, path_hbm, demand_hbm, tail_hbm, cost_hbm, price_hbm, dist_hbm, out_ref,
    path_ref, demand_ref, tail_ref, cost_ref, price_ref, dist_ref, sems,
):
    copies = fetch(
        (
            (path_hbm, path_ref),
            (demand_hbm, demand_ref),
            (tail_hbm, tail_ref),
            (cost_hbm, cost_ref),
            (price_hbm, price_ref),
            (dist_hbm, dist_ref),
        ),
        sems,
    )
    peers = out_ref.shape[0]
    degree, shard_nodes = tail_ref.shape
    shard_blocks = shard_nodes // LANES
    mine = dist_ref.shape[0] // peers
    block_total = node_count // LANES
    routes, hops = path_ref.shape

    copies[0].wait()
    copies[1].wait()
    path = path_ref[...]
    slot = path // node_count
    node = path - slot * node_count
    block = node // LANES
    lane = node - block * LANES
    row = block * degree + slot
    row_total = block_total * degree
    row_ids = lax.broadcasted_iota(jnp.int32, (row_total, hops), 0)
    lane_ids = lax.broadcasted_iota(jnp.int32, (LANES, hops), 0)
    left = [[], [], []]
    right = []
    for k in range(routes):
        hit = row_ids == row[k : k + 1, :]
        amount = jnp.full((1, hops), demand_ref[k], jnp.float32)
        for part, piece in enumerate(three_parts(amount)):
            left[part].append(
                jnp.where(hit, piece.astype(jnp.float32), jnp.float32(0.0)).astype(jnp.bfloat16)
            )
        right.append(
            jnp.where(lane_ids == lane[k : k + 1, :], jnp.float32(1.0), jnp.float32(0.0)).astype(
                jnp.bfloat16
            )
        )
    right = jnp.concatenate(right, axis=1)
    flow = None
    for part in (2, 1, 0):
        term = lax.dot_general(
            jnp.concatenate(left[part], axis=1),
            right,
            (((1,), (1,)), ((), ())),
            preferred_element_type=jnp.float32,
        )
        flow = term if flow is None else flow + term

    for copy in copies[2:]:
        copy.wait()
    tail = tail_ref[...].astype(jnp.float32)
    weight = cost_ref[...] + price_ref[...]
    arc_rows = degree * shard_blocks
    half = degree // 2
    half_rows = half * shard_blocks
    base = mine * shard_blocks
    for j in range(peers):
        slots = slice(j % 2 * half, (j % 2 + 1) * half)
        for b in range(shard_blocks):
            cols = slice(b * LANES, (b + 1) * LANES)
            out_ref[j, b * mine : (b + 1) * mine, :] = dist_ref[j * mine : (j + 1) * mine, cols]
            out_ref[j, base + b * half : base + (b + 1) * half, :] = tail[slots, cols]
            start = base + half_rows + b * half
            out_ref[j, start : start + half, :] = weight[slots, cols]
        start = base + 2 * half_rows
        out_ref[j, start : start + arc_rows, :] = flow[j * arc_rows : (j + 1) * arc_rows, :]


def halo_store(ref, k, half, groups, span, value):
    blocks = groups * SUB
    base = k * span + REACH
    ref[base + half * SUB : base + (half + 1) * SUB, :] = value
    if half == groups - 1:
        ref[base - REACH : base, :] = value[SUB - REACH :, :]
    if half == 0:
        ref[base + blocks : base + blocks + REACH, :] = value[:REACH, :]


def split_kernel(buf_ref, flow_ref, arcs_ref):
    total = None
    rows = flow_ref.shape[0]
    end = buf_ref.shape[1] - rows
    for i in range(buf_ref.shape[0]):
        part = buf_ref[i, end:, :]
        total = part if total is None else total + part
        arcs_ref[i, :, :] = buf_ref[i, end - arcs_ref.shape[1] : end, :]
    flow_ref[...] = total


def plan_rounds(
    degree, block_total, half, stage, stage_w, idx_ref, w_ref, left_idx_ref, left_off_ref, left_w_ref
):
    groups = block_total // SUB
    width = 2 * REACH + 1
    rows = lax.broadcasted_iota(jnp.int32, (SUB, LANES), 0) + half * SUB
    used = jnp.zeros((SUB, LANES), jnp.int32)
    over = jnp.full((SUB, LANES), degree, jnp.int32)
    lanes_of, weights, bits, opens, offs = [], [], [], [], []
    for s in range(degree):
        at = s * (stage.shape[0] // degree) + half * SUB
        tail = stage[at : at + SUB, :].astype(jnp.int32)
        block = tail // LANES
        lane = tail - block * LANES
        off = block - rows + REACH
        off = jnp.where(off < 0, off + block_total, off)
        off = jnp.where(off >= block_total, off - block_total, off)
        weight = stage_w[at : at + SUB, :]
        turned = [jnp.left_shift(1, off)]
        for _ in range(3):
            last = turned[-1]
            turned.append(((last << 1) | (last >> (width - 1))) & (2**width - 1))
        open_rounds = jnp.zeros_like(used)
        for j, (low, high, count) in enumerate(TURNS):
            if low is None:
                spot = turned[0]
            else:
                by_low = ((lane >> low) & 1) == 1
                by_high = ((lane >> high) & 1) == 1
                spot = jnp.where(
                    by_high,
                    jnp.where(by_low, turned[3], turned[2]),
                    jnp.where(by_low, turned[1], turned[0]),
                )
            if count < width:
                spot = spot & (2**count - 1)
            open_rounds = open_rounds | (spot << (width * j))
        free = open_rounds & ~used
        bit = free & -free
        if s >= len(TURNS) - 1:
            near, far = jnp.zeros_like(used), jnp.zeros_like(used)
            for earlier, taken in zip(opens, bits):
                near = near | jnp.where((earlier & ~used) != 0, taken, 0)
            for earlier, taken in zip(opens, bits):
                far = far | jnp.where((earlier & near) != 0, taken, 0)
            straight = open_rounds & near
            wanted = jnp.where(straight != 0, straight, open_rounds & far)
            wanted = jnp.where(bit == 0, wanted & -wanted, 0)
            twice = jnp.where(straight != 0, 0, wanted)
            passed = jnp.zeros_like(used)
            chain = []
            for earlier, taken in zip(opens, bits):
                target = earlier & near
                target = jnp.where((taken & twice) != 0, target & -target, 0)
                passed = passed | target
                chain.append(target)
            last = jnp.where(straight != 0, wanted, passed)
            freed = ~used
            for e, (earlier, taken, target) in enumerate(zip(opens, bits, chain)):
                end = earlier & freed
                end = jnp.where((taken & last) != 0, end & -end, 0)
                used = used | end
                moved = target | end
                bits[e] = jnp.where(moved != 0, moved, taken)
            bit = bit | wanted
        used = used | bit
        over = jnp.minimum(over, jnp.where(bit == 0, s, degree))
        opens.append(open_rounds)
        offs.append(off)
        lanes_of.append(lane)
        weights.append(weight)
        bits.append(bit)
    for s in range(degree):
        at = s * block_total + half * SUB
        left_idx_ref[at : at + SUB, :] = lanes_of[s]
        left_off_ref[at : at + SUB, :] = offs[s]
        left_w_ref[at : at + SUB, :] = jnp.where(bits[s] == 0, weights[s], jnp.float32(jnp.inf))
    for r in range(ROUNDS):
        idx = jnp.zeros((SUB, LANES), jnp.int32)
        weight = jnp.full((SUB, LANES), jnp.inf, jnp.float32)
        for s in range(degree):
            hit = bits[s] == (1 << r)
            idx = jnp.where(hit, lanes_of[s], idx)
            weight = jnp.where(hit, weights[s], weight)
        at = (r * groups + half) * SUB
        idx_ref[at : at + SUB, :] = idx
        w_ref[at : at + SUB, :] = weight
    return over


def sweep_once(mine, degree, first_over, src, dst, tables):
    idx_ref, w_ref, left_idx_ref, left_off_ref, left_w_ref = tables
    span = src.shape[0] // mine
    block_total = span - PAD
    groups = block_total // SUB
    width = 2 * REACH + 1
    lane = lax.broadcasted_iota(jnp.int32, (SUB, LANES), 1)
    bit_masks = [((lane >> t) & 1) == 1 for t in range(LANES.bit_length() - 1)]
    for half in range(groups):
        best = [src[k * span + REACH + half * SUB : k * span + REACH + (half + 1) * SUB, :] for k in range(mine)]
        for j, (low, high, count) in enumerate(TURNS):
            for q in range(count):
                at = ((j * width + q) * groups + half) * SUB
                idx = idx_ref[at : at + SUB, :]
                w = w_ref[at : at + SUB, :]
                for k in range(mine):
                    base = k * span + half * SUB

                    def block(turned):
                        o = base + (q - turned) % width
                        return src[o : o + SUB, :]

                    if low is None:
                        shown = block(0)
                    else:
                        shown = jnp.where(
                            bit_masks[high],
                            jnp.where(bit_masks[low], block(3), block(2)),
                            jnp.where(bit_masks[low], block(1), block(0)),
                        )
                    value = jnp.take_along_axis(shown, idx, axis=1, mode="promise_in_bounds")
                    best[k] = jnp.minimum(best[k], value + w)
        for k in range(mine):
            halo_store(dst, k, half, groups, span, best[k])

    @pl.loop(first_over, degree)
    def _(s):
        for half in range(groups):
            at = pl.multiple_of(s * block_total + half * SUB, SUB)
            idx = left_idx_ref[pl.ds(at, SUB), :]
            off = left_off_ref[pl.ds(at, SUB), :]
            w = left_w_ref[pl.ds(at, SUB), :]
            for k in range(mine):
                base = k * span + REACH + half * SUB
                picked = None
                for o in range(width):
                    start = base + o - REACH
                    value = jnp.take_along_axis(
                        src[start : start + SUB, :], idx, axis=1, mode="promise_in_bounds"
                    )
                    picked = value if picked is None else jnp.where(off == o, value, picked)
                now = dst[base : base + SUB, :]
                halo_store(dst, k, half, groups, span, jnp.minimum(now, picked + w))


def sweep_pairs(count, mine, degree, first_over, one, two, tables):
    @pl.loop(0, count // 2)
    def _(_):
        sweep_once(mine, degree, first_over, one, two, tables)
        sweep_once(mine, degree, first_over, two, one, tables)


def begin_kernel(
    mine, degree, source_hbm, buf_ref, own_ref, partner_ref,
    x_ref, idx_ref, w_ref, left_idx_ref, left_off_ref, left_w_ref, over_ref,
    stage, stage_tail, stage_w, source_ref, sems,
):
    (copy,) = fetch(((source_hbm, source_ref),), sems)
    pitch = stage.shape[0] // mine
    peers = buf_ref.shape[0]
    span = x_ref.shape[0] // mine
    block_total = span - PAD
    groups = block_total // SUB
    shard_blocks = block_total // peers
    half = degree // 2
    for i in range(peers):
        for b in range(shard_blocks):
            blk = i * shard_blocks + b
            stage[pl.ds(blk, mine, stride=pitch), :] = buf_ref[i, b * mine : (b + 1) * mine, :]
            for side, ref in enumerate((own_ref, partner_ref)):
                at = pl.ds(side * half * pitch + blk, half, stride=pitch)
                stage_tail[at, :] = ref[i, b * half : (b + 1) * half, :]
                start = half * shard_blocks + b * half
                stage_w[at, :] = ref[i, start : start + half, :]
    over = None
    for half in range(groups):
        part = plan_rounds(
            degree, block_total, half, stage_tail, stage_w, idx_ref, w_ref,
            left_idx_ref, left_off_ref, left_w_ref,
        )
        over = part if over is None else jnp.minimum(over, part)
    copy.wait()
    rows = lax.broadcasted_iota(jnp.int32, (SUB, LANES), 0)
    lanes = lax.broadcasted_iota(jnp.int32, (SUB, LANES), 1)
    first = lax.axis_index("arc") * mine
    for half in range(groups):
        node = (rows + half * SUB) * LANES + lanes
        for k in range(mine):
            at = k * pitch + half * SUB
            value = jnp.where(node == source_ref[first + k], jnp.float32(0.0), stage[at : at + SUB, :])
            halo_store(x_ref, k, half, groups, span, value)
    over_ref[...] = jnp.full(over_ref.shape, jnp.min(over.astype(jnp.float32)).astype(jnp.int32))


def add_kernel(a_ref, b_ref, after_ref, out_ref):
    out_ref[...] = a_ref[...] + b_ref[...]


def middle_kernel(
    mine, degree, count, over_ref, start_ref, idx_ref, w_ref, left_idx_ref, left_off_ref,
    left_w_ref, x_ref, other,
):
    x_ref[...] = start_ref[...]
    tables = (idx_ref, w_ref, left_idx_ref, left_off_ref, left_w_ref)
    sweep_pairs(count, mine, degree, over_ref[0, 0], x_ref, other, tables)


def end_kernel(
    mine, degree, count, parts, over_ref, start_ref, idx_ref, w_ref, left_idx_ref, left_off_ref,
    left_w_ref, cap_ref, *refs,
):
    flow_refs, (out_ref, grad_ref, x_ref, other) = refs[:parts], refs[parts:]
    peers = out_ref.shape[0]
    span = x_ref.shape[0] // mine
    block_total = span - PAD
    shard_blocks = block_total // peers
    tables = (idx_ref, w_ref, left_idx_ref, left_off_ref, left_w_ref)
    first_over = over_ref[0, 0]
    x_ref[...] = start_ref[...]
    sweep_pairs(count, mine, degree, first_over, x_ref, other, tables)
    square = None
    for b in range(shard_blocks):
        cols = slice(b * LANES, (b + 1) * LANES)
        flow = None
        for ref in flow_refs:
            part = ref[b * degree : (b + 1) * degree, :]
            flow = part if flow is None else flow + part
        grad = flow - cap_ref[:, cols]
        grad_ref[:, cols] = grad
        term = grad * grad
        square = term if square is None else square + term
    folded = jnp.sum(square.reshape(degree // SUB, SUB, LANES), axis=0)
    base = mine * shard_blocks
    for i in range(peers):
        for b in range(shard_blocks):
            blk = REACH + i * shard_blocks + b
            out_ref[i, b * mine : (b + 1) * mine, :] = x_ref[pl.ds(blk, mine, stride=span), :]
        out_ref[i, base : base + SUB, :] = folded


def final_kernel(mine, arc_total, buf_ref, grad_ref, price_ref, dist_ref, new_ref):
    peers = buf_ref.shape[0]
    shard_blocks = dist_ref.shape[1] // LANES
    base = mine * shard_blocks
    total = None
    for i in range(peers):
        for b in range(shard_blocks):
            dist_ref[i * mine : (i + 1) * mine, b * LANES : (b + 1) * LANES] = buf_ref[
                i, b * mine : (b + 1) * mine, :
            ]
        part = buf_ref[i, base : base + SUB, :]
        total = part if total is None else total + part
    square_sum = jnp.sum(jnp.sum(total, axis=1, keepdims=True), axis=0, keepdims=True)
    scale_root = jnp.sqrt(square_sum / arc_total + eps_value)
    new_ref[...] = jnp.maximum(
        price_ref[...] + step_size * grad_ref[...] / scale_root, jnp.float32(0.0)
    )


def shards(prev_dist, source_node, arc_tail, base_cost, arc_price, capacity, path_arcs, demand):
    commodities, shard_nodes = prev_dist.shape
    peers = lax.axis_size("arc")
    groups = lax.axis_size("comm")
    node_count = shard_nodes * peers
    degree = arc_tail.shape[0]
    mine = commodities // peers
    shard_blocks = shard_nodes // LANES
    block_total = node_count // LANES
    span = block_total + PAD
    arc_rows = degree * shard_blocks
    f32, i32 = jnp.float32, jnp.int32
    shape = jax.ShapeDtypeStruct
    near = pltpu.VMEM
    v = vmem_spec

    def held(x):
        return pltpu.with_memory_space_constraint(x, pltpu.VMEM)

    def far(x):
        return pltpu.with_memory_space_constraint(x, pltpu.HBM)

    def scratch(*arrays):
        return [pltpu.VMEM(x.shape, x.dtype) for x in arrays]

    h = functools.partial(pl.BlockSpec, memory_space=pltpu.HBM)
    params = pltpu.CompilerParams(vmem_limit_bytes=VMEM_GRANT)
    arcs = (arc_tail, base_cost, arc_price, prev_dist)
    packed = pl.pallas_call(
        functools.partial(pack_kernel, node_count),
        out_shape=near((peers, mine * shard_blocks + 2 * arc_rows, LANES), f32),
        in_specs=[h()] * 6,
        out_specs=v(),
        scratch_shapes=[
            *scratch(path_arcs),
            pltpu.SMEM(demand.shape, f32),
            *scratch(*arcs),
            pltpu.SemaphoreType.DMA((6,)),
        ],
        compiler_params=params,
        name="pack",
    )(far(path_arcs), far(demand), *map(far, arcs))
    received = held(lax.all_to_all(packed, "arc", 0, 0, tiled=True))

    flow, own = pl.pallas_call(
        split_kernel,
        out_shape=(near((arc_rows, LANES), f32), near((peers, arc_rows, LANES), f32)),
        in_specs=[v()],
        out_specs=(v(), v()),
        compiler_params=params,
        name="split",
    )(received)
    own = held(own)
    partner = held(lax.ppermute(own, "arc", [(i, i ^ 1) for i in range(peers)]))

    def exchange(step):
        pairs = [(i, i ^ (1 << step)) for i in range(groups)]
        return held(lax.ppermute(flow, "comm", pairs))

    steps = groups.bit_length() - 1
    if 1 << steps != groups:
        flow, steps = held(lax.psum(flow, "comm")), 0
    arrived = exchange(0) if steps else None

    rounds = ROUNDS
    table = degree * block_total
    state = (mine * span, LANES)
    x, *tables, over = pl.pallas_call(
        functools.partial(begin_kernel, mine, degree),
        out_shape=(
            near(state, f32),
            near((rounds * block_total, LANES), i32),
            near((rounds * block_total, LANES), f32),
            near((table, LANES), i32),
            near((table, LANES), i32),
            near((table, LANES), f32),
            near((SUB, LANES), i32),
        ),
        in_specs=[h(), v(), v(), v()],
        out_specs=(v(),) * 7,
        scratch_shapes=[
            pltpu.VMEM((mine * (block_total + 1), LANES), f32),
            pltpu.VMEM((degree * (block_total + 1), LANES), f32),
            pltpu.VMEM((degree * (block_total + 1), LANES), f32),
            pltpu.SMEM(source_node.shape, i32),
            pltpu.SemaphoreType.DMA((1,)),
        ],
        compiler_params=params,
        name="begin",
    )(far(source_node), received, own, partner)

    tables, over = tuple(map(held, tables)), held(over)
    left = SWEEPS
    for step in range(1, steps):
        flow = pl.pallas_call(
            add_kernel,
            out_shape=near((arc_rows, LANES), f32),
            in_specs=[v(), v(), v()],
            out_specs=v(),
            compiler_params=params,
            name="add",
        )(held(flow), arrived, held(x))
        arrived = exchange(step)
        count = min(2 if steps > 2 else 4, left - 2)
        left -= count
        x = pl.pallas_call(
            functools.partial(middle_kernel, mine, degree, count),
            out_shape=near(state, f32),
            in_specs=[v()] * (len(tables) + 2),
            out_specs=v(),
            scratch_shapes=[pltpu.VMEM(state, f32)],
            compiler_params=params,
                name="middle",
        )(over, held(x), *tables)

    flows = (held(flow),) if arrived is None else (held(flow), arrived)
    back, gradient = pl.pallas_call(
        functools.partial(end_kernel, mine, degree, left, len(flows)),
        out_shape=(
            near((peers, mine * shard_blocks + SUB, LANES), f32),
            near((degree, shard_nodes), f32),
        ),
        in_specs=[v()] * (len(tables) + 3 + len(flows)),
        out_specs=(v(), v()),
        scratch_shapes=[pltpu.VMEM(state, f32), pltpu.VMEM(state, f32)],
        compiler_params=params,
        name="end",
    )(over, held(x), *tables, capacity, *flows)
    final = held(lax.all_to_all(back, "arc", 0, 0, tiled=True))
    return pl.pallas_call(
        functools.partial(final_kernel, mine, degree * node_count),
        out_shape=(shape((commodities, shard_nodes), f32), shape((degree, shard_nodes), f32)),
        in_specs=[v(), v(), v()],
        out_specs=(v(), v()),
        compiler_params=params,
        name="finish",
    )(final, held(gradient), arc_price)


def solution(mesh):
    in_specs = (
        P("comm", "arc"),
        P("comm"),
        P(None, "arc"),
        P(None, "arc"),
        P(None, "arc"),
        P(None, "arc"),
        P(("comm", "arc"), None),
        P(("comm", "arc")),
    )
    out_specs = (P("comm", "arc"), P(None, "arc"))
    return jax.shard_map(shards, mesh=mesh, in_specs=in_specs, out_specs=out_specs, check_vma=False)
```

```python
import functools

import jax
import jax.numpy as jnp
from jax import lax
from jax.experimental import pallas as pl
from jax.experimental.pallas import tpu as pltpu
from jax.sharding import PartitionSpec as P

SWEEPS = 8
REACH = 2
LANES = 128
SUB = 8
PAD = 2 * REACH + 1
VMEM_GRANT = 24 * 1024 * 1024

TURNS = ((None, None, 5), (0, 1, 5), (2, 3, 5), (4, 5, 5), (6, 0, 2))
ROUNDS = sum(turn[2] for turn in TURNS)

step_size = 0.25
eps_value = 1e-06


def vmem_spec():
    return pl.BlockSpec(memory_space=pltpu.VMEM)


def three_parts(x):
    first = x.astype(jnp.bfloat16)
    rest = x - first.astype(jnp.float32)
    second = rest.astype(jnp.bfloat16)
    third = (rest - second.astype(jnp.float32)).astype(jnp.bfloat16)
    return first, second, third


def fetch(pairs, sems):
    copies = [pltpu.make_async_copy(src, dst, sems.at[n]) for n, (src, dst) in enumerate(pairs)]
    for copy in copies:
        copy.start()
    return copies


def pack_kernel(
    node_count, path_hbm, demand_hbm, tail_hbm, cost_hbm, price_hbm, dist_hbm, out_ref,
    path_ref, demand_ref, tail_ref, cost_ref, price_ref, dist_ref, sems,
):
    copies = fetch(
        (
            (path_hbm, path_ref),
            (demand_hbm, demand_ref),
            (tail_hbm, tail_ref),
            (cost_hbm, cost_ref),
            (price_hbm, price_ref),
            (dist_hbm, dist_ref),
        ),
        sems,
    )
    peers = 2 * out_ref.shape[0]
    degree, shard_nodes = tail_ref.shape
    shard_blocks = shard_nodes // LANES
    mine = dist_ref.shape[0] // peers
    block_total = node_count // LANES
    routes, hops = path_ref.shape

    copies[0].wait()
    copies[1].wait()
    path = path_ref[...]
    slot = path // node_count
    node = path - slot * node_count
    block = node // LANES
    lane = node - block * LANES
    row = block * degree + slot
    row_total = block_total * degree
    row_ids = lax.broadcasted_iota(jnp.int32, (row_total, hops), 0)
    lane_ids = lax.broadcasted_iota(jnp.int32, (LANES, hops), 0)
    left = [[], [], []]
    right = []
    for k in range(routes):
        hit = row_ids == row[k : k + 1, :]
        amount = jnp.full((1, hops), demand_ref[k], jnp.float32)
        for part, piece in enumerate(three_parts(amount)):
            left[part].append(
                jnp.where(hit, piece.astype(jnp.float32), jnp.float32(0.0)).astype(jnp.bfloat16)
            )
        right.append(
            jnp.where(lane_ids == lane[k : k + 1, :], jnp.float32(1.0), jnp.float32(0.0)).astype(
                jnp.bfloat16
            )
        )
    right = jnp.concatenate(right, axis=1)
    flow = None
    for part in (2, 1, 0):
        term = lax.dot_general(
            jnp.concatenate(left[part], axis=1),
            right,
            (((1,), (1,)), ((), ())),
            preferred_element_type=jnp.float32,
        )
        flow = term if flow is None else flow + term

    for copy in copies[2:]:
        copy.wait()
    tail = tail_ref[...].astype(jnp.float32)
    weight = cost_ref[...] + price_ref[...]
    arc_rows = degree * shard_blocks
    dist_rows = mine * shard_blocks
    even = lax.axis_index("arc") % 2 == 0
    for pair in range(peers // 2):
        for b in range(shard_blocks):
            cols = slice(b * LANES, (b + 1) * LANES)
            first, second = (
                dist_ref[j * mine : (j + 1) * mine, cols] for j in (2 * pair, 2 * pair + 1)
            )
            at = b * mine
            out_ref[pair, at : at + mine, :] = jnp.where(even, first, second)
            at = dist_rows + b * degree
            out_ref[pair, at : at + degree, :] = tail[:, cols]
            at = at + arc_rows
            out_ref[pair, at : at + degree, :] = weight[:, cols]
            at = dist_rows + 2 * arc_rows + b * mine
            out_ref[pair, at : at + mine, :] = jnp.where(even, second, first)
        first, second = (
            flow[j * arc_rows : (j + 1) * arc_rows, :] for j in (2 * pair, 2 * pair + 1)
        )
        at = 2 * dist_rows + 2 * arc_rows
        out_ref[pair, at : at + arc_rows, :] = jnp.where(even, first, second)
        at = at + arc_rows
        out_ref[pair, at : at + arc_rows, :] = jnp.where(even, second, first)


def halo_store(ref, k, half, groups, span, value):
    blocks = groups * SUB
    base = k * span + REACH
    ref[base + half * SUB : base + (half + 1) * SUB, :] = value
    if half == groups - 1:
        ref[base - REACH : base, :] = value[SUB - REACH :, :]
    if half == 0:
        ref[base + blocks : base + blocks + REACH, :] = value[:REACH, :]


def split_kernel(buf_ref, flow_ref, pass_ref):
    total = None
    end = buf_ref.shape[1] - flow_ref.shape[0]
    for i in range(buf_ref.shape[0]):
        part = buf_ref[i, end:, :]
        total = part if total is None else total + part
        pass_ref[i, :, :] = buf_ref[i, end - pass_ref.shape[1] : end, :]
    flow_ref[...] = total


def plan_rounds(
    degree, block_total, half, stage, stage_w, idx_ref, w_ref, left_idx_ref, left_off_ref, left_w_ref
):
    groups = block_total // SUB
    width = 2 * REACH + 1
    rows = lax.broadcasted_iota(jnp.int32, (SUB, LANES), 0) + half * SUB
    used = jnp.zeros((SUB, LANES), jnp.int32)
    over = jnp.full((SUB, LANES), degree, jnp.int32)
    lanes_of, weights, bits, opens, offs = [], [], [], [], []
    for s in range(degree):
        at = s * (stage.shape[0] // degree) + half * SUB
        tail = stage[at : at + SUB, :].astype(jnp.int32)
        block = tail // LANES
        lane = tail - block * LANES
        off = block - rows + REACH
        off = jnp.where(off < 0, off + block_total, off)
        off = jnp.where(off >= block_total, off - block_total, off)
        weight = stage_w[at : at + SUB, :]
        turned = [jnp.left_shift(1, off)]
        for _ in range(3):
            last = turned[-1]
            turned.append(((last << 1) | (last >> (width - 1))) & (2**width - 1))
        open_rounds = jnp.zeros_like(used)
        for j, (low, high, count) in enumerate(TURNS):
            if low is None:
                spot = turned[0]
            else:
                by_low = ((lane >> low) & 1) == 1
                by_high = ((lane >> high) & 1) == 1
                spot = jnp.where(
                    by_high,
                    jnp.where(by_low, turned[3], turned[2]),
                    jnp.where(by_low, turned[1], turned[0]),
                )
            if count < width:
                spot = spot & (2**count - 1)
            open_rounds = open_rounds | (spot << (width * j))
        free = open_rounds & ~used
        bit = free & -free
        if s >= len(TURNS) - 1:
            near, far = jnp.zeros_like(used), jnp.zeros_like(used)
            for earlier, taken in zip(opens, bits):
                near = near | jnp.where((earlier & ~used) != 0, taken, 0)
            for earlier, taken in zip(opens, bits):
                far = far | jnp.where((earlier & near) != 0, taken, 0)
            straight = open_rounds & near
            wanted = jnp.where(straight != 0, straight, open_rounds & far)
            wanted = jnp.where(bit == 0, wanted & -wanted, 0)
            twice = jnp.where((straight != 0) | (wanted == 0), -1, wanted)
            passed = jnp.zeros_like(used)
            for earlier, taken in zip(opens, bits):
                passed = passed | jnp.where(taken == twice, earlier, 0)
            passed = passed & near
            passed = passed & -passed
            last = passed | jnp.where(straight != 0, wanted, 0)
            last = jnp.where(last == 0, -1, last)
            end = jnp.zeros_like(used)
            for earlier, taken in zip(opens, bits):
                end = end | jnp.where(taken == last, earlier, 0)
            end = end & ~used
            end = end & -end
            used = used | end
            for e, taken in enumerate(bits):
                bits[e] = jnp.where(taken == last, end, jnp.where(taken == twice, passed, taken))
            bit = bit | wanted
        used = used | bit
        over = jnp.minimum(over, jnp.where(bit == 0, s, degree))
        opens.append(open_rounds)
        offs.append(off)
        lanes_of.append(lane)
        weights.append(weight)
        bits.append(bit)
    for s in range(degree):
        at = s * block_total + half * SUB
        left_idx_ref[at : at + SUB, :] = lanes_of[s]
        left_off_ref[at : at + SUB, :] = offs[s]
        left_w_ref[at : at + SUB, :] = jnp.where(bits[s] == 0, weights[s], jnp.float32(jnp.inf))
    for r in range(ROUNDS):
        idx = jnp.zeros((SUB, LANES), jnp.int32)
        weight = jnp.full((SUB, LANES), jnp.inf, jnp.float32)
        for s in range(degree):
            hit = bits[s] == (1 << r)
            idx = jnp.where(hit, lanes_of[s], idx)
            weight = jnp.where(hit, weights[s], weight)
        at = (r * groups + half) * SUB
        idx_ref[at : at + SUB, :] = idx
        w_ref[at : at + SUB, :] = weight
    return over


def sweep_once(mine, degree, first_over, src, dst, tables):
    idx_ref, w_ref, left_idx_ref, left_off_ref, left_w_ref = tables
    span = src.shape[0] // mine
    block_total = span - PAD
    groups = block_total // SUB
    width = 2 * REACH + 1
    lane = lax.broadcasted_iota(jnp.int32, (SUB, LANES), 1)
    bit_masks = [((lane >> t) & 1) == 1 for t in range(LANES.bit_length() - 1)]
    for half in range(groups):
        best = [src[k * span + REACH + half * SUB : k * span + REACH + (half + 1) * SUB, :] for k in range(mine)]
        for j, (low, high, count) in enumerate(TURNS):
            for q in range(count):
                at = ((j * width + q) * groups + half) * SUB
                idx = idx_ref[at : at + SUB, :]
                w = w_ref[at : at + SUB, :]
                for k in range(mine):
                    base = k * span + half * SUB

                    def block(turned):
                        o = base + (q - turned) % width
                        return src[o : o + SUB, :]

                    if low is None:
                        shown = block(0)
                    else:
                        shown = jnp.where(
                            bit_masks[high],
                            jnp.where(bit_masks[low], block(3), block(2)),
                            jnp.where(bit_masks[low], block(1), block(0)),
                        )
                    value = jnp.take_along_axis(shown, idx, axis=1, mode="promise_in_bounds")
                    best[k] = jnp.minimum(best[k], value + w)
        for k in range(mine):
            halo_store(dst, k, half, groups, span, best[k])

    @pl.loop(first_over, degree)
    def _(s):
        for half in range(groups):
            at = pl.multiple_of(s * block_total + half * SUB, SUB)
            idx = left_idx_ref[pl.ds(at, SUB), :]
            off = left_off_ref[pl.ds(at, SUB), :]
            w = left_w_ref[pl.ds(at, SUB), :]
            for k in range(mine):
                base = k * span + REACH + half * SUB
                picked = None
                for o in range(width):
                    start = base + o - REACH
                    value = jnp.take_along_axis(
                        src[start : start + SUB, :], idx, axis=1, mode="promise_in_bounds"
                    )
                    picked = value if picked is None else jnp.where(off == o, value, picked)
                now = dst[base : base + SUB, :]
                halo_store(dst, k, half, groups, span, jnp.minimum(now, picked + w))


def sweep_pairs(count, mine, degree, first_over, one, two, tables):
    @pl.loop(0, count // 2)
    def _(_):
        sweep_once(mine, degree, first_over, one, two, tables)
        sweep_once(mine, degree, first_over, two, one, tables)


def begin_kernel(
    mine, degree, source_hbm, buf_ref, partner_ref,
    x_ref, idx_ref, w_ref, left_idx_ref, left_off_ref, left_w_ref, over_ref,
    stage, stage_tail, stage_w, source_ref, sems,
):
    (copy,) = fetch(((source_hbm, source_ref),), sems)
    pitch = stage.shape[0] // mine
    peers = 2 * buf_ref.shape[0]
    span = x_ref.shape[0] // mine
    block_total = span - PAD
    groups = block_total // SUB
    shard_blocks = block_total // peers
    arc_rows = degree * shard_blocks
    dist_rows = mine * shard_blocks
    even = lax.axis_index("arc") % 2 == 0

    def unpack(target, i, b, rows, own_at, partner_at):
        own = buf_ref[i, own_at + b * rows : own_at + (b + 1) * rows, :]
        partner = partner_ref[i, partner_at + b * rows : partner_at + (b + 1) * rows, :]
        blk = 2 * i * shard_blocks + b
        target[pl.ds(blk, rows, stride=pitch), :] = jnp.where(even, own, partner)
        blk = blk + shard_blocks
        target[pl.ds(blk, rows, stride=pitch), :] = jnp.where(even, partner, own)

    for i in range(peers // 2):
        for b in range(shard_blocks):
            unpack(stage, i, b, mine, 0, 2 * arc_rows)
            unpack(stage_tail, i, b, degree, dist_rows, 0)
            unpack(stage_w, i, b, degree, dist_rows + arc_rows, arc_rows)
    over = None
    for half in range(groups):
        part = plan_rounds(
            degree, block_total, half, stage_tail, stage_w, idx_ref, w_ref,
            left_idx_ref, left_off_ref, left_w_ref,
        )
        over = part if over is None else jnp.minimum(over, part)
    copy.wait()
    rows = lax.broadcasted_iota(jnp.int32, (SUB, LANES), 0)
    lanes = lax.broadcasted_iota(jnp.int32, (SUB, LANES), 1)
    first = lax.axis_index("arc") * mine
    for half in range(groups):
        node = (rows + half * SUB) * LANES + lanes
        for k in range(mine):
            at = k * pitch + half * SUB
            value = jnp.where(node == source_ref[first + k], jnp.float32(0.0), stage[at : at + SUB, :])
            halo_store(x_ref, k, half, groups, span, value)
    over_ref[...] = jnp.full(over_ref.shape, jnp.min(over.astype(jnp.float32)).astype(jnp.int32))


def merge_kernel(a_ref, b_ref, after_ref, *out_refs):
    total = a_ref[...] + b_ref[...]
    for n, ref in enumerate(out_refs):
        rows = ref.shape[0]
        ref[...] = total[n * rows : (n + 1) * rows, :]


def middle_kernel(
    mine, degree, count, over_ref, start_ref, idx_ref, w_ref, left_idx_ref, left_off_ref,
    left_w_ref, x_ref, other,
):
    x_ref[...] = start_ref[...]
    tables = (idx_ref, w_ref, left_idx_ref, left_off_ref, left_w_ref)
    sweep_pairs(count, mine, degree, over_ref[0, 0], x_ref, other, tables)


def end_kernel(
    mine, degree, count, parts, over_ref, start_ref, idx_ref, w_ref, left_idx_ref, left_off_ref,
    left_w_ref, cap_ref, *refs,
):
    flow_refs, (out_ref, grad_ref, x_ref, other) = refs[:parts], refs[parts:]
    peers = out_ref.shape[0]
    span = x_ref.shape[0] // mine
    block_total = span - PAD
    shard_blocks = block_total // peers
    tables = (idx_ref, w_ref, left_idx_ref, left_off_ref, left_w_ref)
    first_over = over_ref[0, 0]
    x_ref[...] = start_ref[...]
    sweep_pairs(count, mine, degree, first_over, x_ref, other, tables)
    square = None
    for b in range(shard_blocks):
        cols = slice(b * LANES, (b + 1) * LANES)
        flow = None
        for ref in flow_refs:
            part = ref[b * degree : (b + 1) * degree, :]
            flow = part if flow is None else flow + part
        grad = flow - cap_ref[:, cols]
        grad_ref[:, cols] = grad
        term = grad * grad
        square = term if square is None else square + term
    folded = jnp.sum(square.reshape(degree // SUB, SUB, LANES), axis=0)
    base = mine * shard_blocks
    for i in range(peers):
        for b in range(shard_blocks):
            blk = REACH + i * shard_blocks + b
            out_ref[i, b * mine : (b + 1) * mine, :] = x_ref[pl.ds(blk, mine, stride=span), :]
        out_ref[i, base : base + SUB, :] = folded


def final_kernel(mine, arc_total, buf_ref, grad_ref, price_ref, dist_ref, new_ref):
    peers = buf_ref.shape[0]
    shard_blocks = dist_ref.shape[1] // LANES
    base = mine * shard_blocks
    total = None
    for i in range(peers):
        for b in range(shard_blocks):
            dist_ref[i * mine : (i + 1) * mine, b * LANES : (b + 1) * LANES] = buf_ref[
                i, b * mine : (b + 1) * mine, :
            ]
        part = buf_ref[i, base : base + SUB, :]
        total = part if total is None else total + part
    square_sum = jnp.sum(jnp.sum(total, axis=1, keepdims=True), axis=0, keepdims=True)
    scale_root = jnp.sqrt(square_sum / arc_total + eps_value)
    new_ref[...] = jnp.maximum(
        price_ref[...] + step_size * grad_ref[...] / scale_root, jnp.float32(0.0)
    )


def shards(prev_dist, source_node, arc_tail, base_cost, arc_price, capacity, path_arcs, demand):
    commodities, shard_nodes = prev_dist.shape
    peers = lax.axis_size("arc")
    groups = lax.axis_size("comm")
    node_count = shard_nodes * peers
    degree = arc_tail.shape[0]
    mine = commodities // peers
    shard_blocks = shard_nodes // LANES
    block_total = node_count // LANES
    span = block_total + PAD
    arc_rows = degree * shard_blocks
    f32, i32 = jnp.float32, jnp.int32
    shape = jax.ShapeDtypeStruct
    near = pltpu.VMEM
    v = vmem_spec

    def held(x):
        return pltpu.with_memory_space_constraint(x, pltpu.VMEM)

    def far(x):
        return pltpu.with_memory_space_constraint(x, pltpu.HBM)

    def scratch(*arrays):
        return [pltpu.VMEM(x.shape, x.dtype) for x in arrays]

    h = functools.partial(pl.BlockSpec, memory_space=pltpu.HBM)
    params = pltpu.CompilerParams(vmem_limit_bytes=VMEM_GRANT)
    arcs = (arc_tail, base_cost, arc_price, prev_dist)
    packed = pl.pallas_call(
        functools.partial(pack_kernel, node_count),
        out_shape=near((peers // 2, 2 * mine * shard_blocks + 4 * arc_rows, LANES), f32),
        in_specs=[h()] * 6,
        out_specs=v(),
        scratch_shapes=[
            *scratch(path_arcs),
            pltpu.SMEM(demand.shape, f32),
            *scratch(*arcs),
            pltpu.SemaphoreType.DMA((6,)),
        ],
        compiler_params=params,
        name="pack",
    )(far(path_arcs), far(demand), *map(far, arcs))
    parities = [list(range(side, peers, 2)) for side in range(2)]
    received = held(
        lax.all_to_all(packed, "arc", 0, 0, tiled=True, axis_index_groups=parities)
    )

    def swap(x):
        return held(lax.ppermute(x, "arc", [(i, i ^ 1) for i in range(peers)]))

    def exchange(x, step):
        pairs = [(i, i ^ (1 << step)) for i in range(groups)]
        return held(lax.ppermute(x, "comm", pairs))

    def merge(a, b, after, parts):
        return pl.pallas_call(
            merge_kernel,
            out_shape=(near((arc_rows, LANES), f32),) * parts,
            in_specs=[v(), v(), v()],
            out_specs=(v(),) * parts,
            compiler_params=params,
            name="merge",
        )(held(a), b, held(after))

    flow, passed = pl.pallas_call(
        split_kernel,
        out_shape=(
            near((2 * arc_rows, LANES), f32),
            near((peers // 2, 2 * arc_rows + mine * shard_blocks, LANES), f32),
        ),
        in_specs=[v()],
        out_specs=(v(), v()),
        compiler_params=params,
        name="split",
    )(received)
    partner = swap(held(passed))

    steps = groups.bit_length() - 1
    if 1 << steps != groups:
        flow, steps = held(lax.psum(flow, "comm")), 0
    arrived = exchange(flow, 0) if steps else jnp.zeros_like(flow)

    rounds = ROUNDS
    table = degree * block_total
    state = (mine * span, LANES)
    x, *tables, over = pl.pallas_call(
        functools.partial(begin_kernel, mine, degree),
        out_shape=(
            near(state, f32),
            near((rounds * block_total, LANES), i32),
            near((rounds * block_total, LANES), f32),
            near((table, LANES), i32),
            near((table, LANES), i32),
            near((table, LANES), f32),
            near((SUB, LANES), i32),
        ),
        in_specs=[h(), v(), v()],
        out_specs=(v(),) * 7,
        scratch_shapes=[
            pltpu.VMEM((mine * (block_total + 1), LANES), f32),
            pltpu.VMEM((degree * (block_total + 1), LANES), f32),
            pltpu.VMEM((degree * (block_total + 1), LANES), f32),
            pltpu.SMEM(source_node.shape, i32),
            pltpu.SemaphoreType.DMA((1,)),
        ],
        compiler_params=params,
        name="begin",
    )(far(source_node), received, partner)

    tables, over = tuple(map(held, tables)), held(over)
    flow, other = merge(flow, held(arrived), x, 2)
    arrived = swap(held(other))
    left = SWEEPS
    for step in range(1, max(steps, 1) + 1):
        count = min(2 if step < steps else 4, left - 2)
        left -= count
        x = pl.pallas_call(
            functools.partial(middle_kernel, mine, degree, count),
            out_shape=near(state, f32),
            in_specs=[v()] * (len(tables) + 2),
            out_specs=v(),
            scratch_shapes=[pltpu.VMEM(state, f32)],
            compiler_params=params,
            name="middle",
        )(over, held(x), *tables)
        if step < steps:
            (flow,) = merge(flow, arrived, x, 1)
            arrived = exchange(held(flow), step)

    flows = (held(flow), arrived)
    back, gradient = pl.pallas_call(
        functools.partial(end_kernel, mine, degree, left, len(flows)),
        out_shape=(
            near((peers, mine * shard_blocks + SUB, LANES), f32),
            near((degree, shard_nodes), f32),
        ),
        in_specs=[v()] * (len(tables) + 3 + len(flows)),
        out_specs=(v(), v()),
        scratch_shapes=[pltpu.VMEM(state, f32), pltpu.VMEM(state, f32)],
        compiler_params=params,
        name="end",
    )(over, held(x), *tables, capacity, *flows)
    final = held(lax.all_to_all(back, "arc", 0, 0, tiled=True))
    return pl.pallas_call(
        functools.partial(final_kernel, mine, degree * node_count),
        out_shape=(shape((commodities, shard_nodes), f32), shape((degree, shard_nodes), f32)),
        in_specs=[v(), v(), v()],
        out_specs=(v(), v()),
        compiler_params=params,
        name="finish",
    )(final, held(gradient), arc_price)


def solution(mesh):
    in_specs = (
        P("comm", "arc"),
        P("comm"),
        P(None, "arc"),
        P(None, "arc"),
        P(None, "arc"),
        P(None, "arc"),
        P(("comm", "arc"), None),
        P(("comm", "arc")),
    )
    out_specs = (P("comm", "arc"), P(None, "arc"))
    return jax.shard_map(shards, mesh=mesh, in_specs=in_specs, out_specs=out_specs, check_vma=False)
```

```python
import functools

import jax
import jax.numpy as jnp
from jax import lax
from jax.experimental import pallas as pl
from jax.experimental.pallas import tpu as pltpu
from jax.sharding import PartitionSpec as P

SWEEPS = 8
REACH = 2
LANES = 128
SUB = 8
PAD = 2 * REACH + 1
VMEM_GRANT = 24 * 1024 * 1024

TURNS = ((None, None, 5), (0, 1, 5), (2, 3, 5), (4, 5, 5), (6, 0, 2))
ROUNDS = sum(turn[2] for turn in TURNS)

step_size = 0.25
eps_value = 1e-06


def vmem_spec():
    return pl.BlockSpec(memory_space=pltpu.VMEM)


def three_parts(x):
    first = x.astype(jnp.bfloat16)
    rest = x - first.astype(jnp.float32)
    second = rest.astype(jnp.bfloat16)
    third = (rest - second.astype(jnp.float32)).astype(jnp.bfloat16)
    return first, second, third


def fetch(pairs, sems):
    copies = [pltpu.make_async_copy(src, dst, sems.at[n]) for n, (src, dst) in enumerate(pairs)]
    for copy in copies:
        copy.start()
    return copies


def pack_kernel(
    node_count, path_hbm, demand_hbm, tail_hbm, cost_hbm, price_hbm, dist_hbm, out_ref,
    path_ref, demand_ref, tail_ref, cost_ref, price_ref, dist_ref, sems,
):
    copies = fetch(
        (
            (path_hbm, path_ref),
            (demand_hbm, demand_ref),
            (tail_hbm, tail_ref),
            (cost_hbm, cost_ref),
            (price_hbm, price_ref),
            (dist_hbm, dist_ref),
        ),
        sems,
    )
    peers = 2 * out_ref.shape[0]
    degree, shard_nodes = tail_ref.shape
    shard_blocks = shard_nodes // LANES
    mine = dist_ref.shape[0] // peers
    block_total = node_count // LANES
    routes, hops = path_ref.shape

    copies[0].wait()
    copies[1].wait()
    path = path_ref[...]
    slot = path // node_count
    node = path - slot * node_count
    block = node // LANES
    lane = node - block * LANES
    row = block * degree + slot
    row_total = block_total * degree
    row_ids = lax.broadcasted_iota(jnp.int32, (row_total, hops), 0)
    lane_ids = lax.broadcasted_iota(jnp.int32, (LANES, hops), 0)
    left = [[], [], []]
    right = []
    for k in range(routes):
        hit = row_ids == row[k : k + 1, :]
        amount = jnp.full((1, hops), demand_ref[k], jnp.float32)
        for part, piece in enumerate(three_parts(amount)):
            left[part].append(
                jnp.where(hit, piece.astype(jnp.float32), jnp.float32(0.0)).astype(jnp.bfloat16)
            )
        right.append(
            jnp.where(lane_ids == lane[k : k + 1, :], jnp.float32(1.0), jnp.float32(0.0)).astype(
                jnp.bfloat16
            )
        )
    right = jnp.concatenate(right, axis=1)
    flow = None
    for part in (2, 1, 0):
        term = lax.dot_general(
            jnp.concatenate(left[part], axis=1),
            right,
            (((1,), (1,)), ((), ())),
            preferred_element_type=jnp.float32,
        )
        flow = term if flow is None else flow + term

    for copy in copies[2:]:
        copy.wait()
    tail = tail_ref[...].astype(jnp.float32)
    weight = cost_ref[...] + price_ref[...]
    arc_rows = degree * shard_blocks
    dist_rows = mine * shard_blocks
    even = lax.axis_index("arc") % 2 == 0
    for pair in range(peers // 2):
        for b in range(shard_blocks):
            cols = slice(b * LANES, (b + 1) * LANES)
            first, second = (
                dist_ref[j * mine : (j + 1) * mine, cols] for j in (2 * pair, 2 * pair + 1)
            )
            at = b * mine
            out_ref[pair, at : at + mine, :] = jnp.where(even, first, second)
            at = dist_rows + b * degree
            out_ref[pair, at : at + degree, :] = tail[:, cols]
            at = at + arc_rows
            out_ref[pair, at : at + degree, :] = weight[:, cols]
            at = dist_rows + 2 * arc_rows + b * mine
            out_ref[pair, at : at + mine, :] = jnp.where(even, second, first)
        first, second = (
            flow[j * arc_rows : (j + 1) * arc_rows, :] for j in (2 * pair, 2 * pair + 1)
        )
        at = 2 * dist_rows + 2 * arc_rows
        out_ref[pair, at : at + arc_rows, :] = jnp.where(even, first, second)
        at = at + arc_rows
        out_ref[pair, at : at + arc_rows, :] = jnp.where(even, second, first)


def halo_store(ref, k, half, groups, span, value):
    blocks = groups * SUB
    base = k * span + REACH
    ref[base + half * SUB : base + (half + 1) * SUB, :] = value
    if half == groups - 1:
        ref[base - REACH : base, :] = value[SUB - REACH :, :]
    if half == 0:
        ref[base + blocks : base + blocks + REACH, :] = value[:REACH, :]


def split_kernel(buf_ref, flow_ref, pass_ref):
    total = None
    end = buf_ref.shape[1] - flow_ref.shape[0]
    for i in range(buf_ref.shape[0]):
        part = buf_ref[i, end:, :]
        total = part if total is None else total + part
        pass_ref[i, :, :] = buf_ref[i, end - pass_ref.shape[1] : end, :]
    flow_ref[...] = total


def plan_rounds(
    degree, block_total, half, stage, stage_w, idx_ref, w_ref, left_idx_ref, left_off_ref, left_w_ref
):
    groups = block_total // SUB
    width = 2 * REACH + 1
    rows = lax.broadcasted_iota(jnp.int32, (SUB, LANES), 0) + half * SUB
    used = jnp.zeros((SUB, LANES), jnp.int32)
    over = jnp.full((SUB, LANES), degree, jnp.int32)
    lanes_of, weights, bits, opens, offs = [], [], [], [], []
    for s in range(degree):
        at = s * (stage.shape[0] // degree) + half * SUB
        tail = stage[at : at + SUB, :].astype(jnp.int32)
        block = tail // LANES
        lane = tail - block * LANES
        off = block - rows + REACH
        off = jnp.where(off < 0, off + block_total, off)
        off = jnp.where(off >= block_total, off - block_total, off)
        weight = stage_w[at : at + SUB, :]
        turned = [jnp.left_shift(1, off)]
        for _ in range(3):
            last = turned[-1]
            turned.append(((last << 1) | (last >> (width - 1))) & (2**width - 1))
        open_rounds = jnp.zeros_like(used)
        for j, (low, high, count) in enumerate(TURNS):
            if low is None:
                spot = turned[0]
            else:
                by_low = ((lane >> low) & 1) == 1
                by_high = ((lane >> high) & 1) == 1
                spot = jnp.where(
                    by_high,
                    jnp.where(by_low, turned[3], turned[2]),
                    jnp.where(by_low, turned[1], turned[0]),
                )
            if count < width:
                spot = spot & (2**count - 1)
            open_rounds = open_rounds | (spot << (width * j))
        free = open_rounds & ~used
        bit = free & -free
        if s >= len(TURNS) - 1:
            near, far = jnp.zeros_like(used), jnp.zeros_like(used)
            for earlier, taken in zip(opens, bits):
                near = near | jnp.where((earlier & ~used) != 0, taken, 0)
            for earlier, taken in zip(opens, bits):
                far = far | jnp.where((earlier & near) != 0, taken, 0)
            straight = open_rounds & near
            wanted = jnp.where(straight != 0, straight, open_rounds & far)
            wanted = jnp.where(bit == 0, wanted & -wanted, 0)
            twice = jnp.where((straight != 0) | (wanted == 0), -1, wanted)
            passed = jnp.zeros_like(used)
            for earlier, taken in zip(opens, bits):
                passed = passed | jnp.where(taken == twice, earlier, 0)
            passed = passed & near
            passed = passed & -passed
            last = passed | jnp.where(straight != 0, wanted, 0)
            last = jnp.where(last == 0, -1, last)
            end = jnp.zeros_like(used)
            for earlier, taken in zip(opens, bits):
                end = end | jnp.where(taken == last, earlier, 0)
            end = end & ~used
            end = end & -end
            used = used | end
            for e, taken in enumerate(bits):
                bits[e] = jnp.where(taken == last, end, jnp.where(taken == twice, passed, taken))
            bit = bit | wanted
        used = used | bit
        over = jnp.minimum(over, jnp.where(bit == 0, s, degree))
        opens.append(open_rounds)
        offs.append(off)
        lanes_of.append(lane)
        weights.append(weight)
        bits.append(bit)
    for s in range(degree):
        at = s * block_total + half * SUB
        left_idx_ref[at : at + SUB, :] = lanes_of[s]
        left_off_ref[at : at + SUB, :] = offs[s]
        left_w_ref[at : at + SUB, :] = jnp.where(bits[s] == 0, weights[s], jnp.float32(jnp.inf))
    for r in range(ROUNDS):
        idx = jnp.zeros((SUB, LANES), jnp.int32)
        weight = jnp.full((SUB, LANES), jnp.inf, jnp.float32)
        for s in range(degree):
            hit = bits[s] == (1 << r)
            idx = jnp.where(hit, lanes_of[s], idx)
            weight = jnp.where(hit, weights[s], weight)
        at = (r * groups + half) * SUB
        idx_ref[at : at + SUB, :] = idx
        w_ref[at : at + SUB, :] = weight
    return over


def sweep_once(mine, degree, first_over, src, dst, tables):
    idx_ref, w_ref, left_idx_ref, left_off_ref, left_w_ref = tables
    span = src.shape[0] // mine
    block_total = span - PAD
    groups = block_total // SUB
    width = 2 * REACH + 1
    lane = lax.broadcasted_iota(jnp.int32, (SUB, LANES), 1)
    bit_masks = [((lane >> t) & 1) == 1 for t in range(LANES.bit_length() - 1)]
    for half in range(groups):
        best = [src[k * span + REACH + half * SUB : k * span + REACH + (half + 1) * SUB, :] for k in range(mine)]
        for j, (low, high, count) in enumerate(TURNS):
            for q in range(count):
                at = ((j * width + q) * groups + half) * SUB
                idx = idx_ref[at : at + SUB, :]
                w = w_ref[at : at + SUB, :]
                for k in range(mine):
                    base = k * span + half * SUB

                    def block(turned):
                        o = base + (q - turned) % width
                        return src[o : o + SUB, :]

                    if low is None:
                        shown = block(0)
                    else:
                        shown = jnp.where(
                            bit_masks[high],
                            jnp.where(bit_masks[low], block(3), block(2)),
                            jnp.where(bit_masks[low], block(1), block(0)),
                        )
                    value = jnp.take_along_axis(shown, idx, axis=1, mode="promise_in_bounds")
                    best[k] = jnp.minimum(best[k], value + w)
        for k in range(mine):
            halo_store(dst, k, half, groups, span, best[k])

    @pl.loop(first_over, degree)
    def _(s):
        for half in range(groups):
            at = pl.multiple_of(s * block_total + half * SUB, SUB)
            idx = left_idx_ref[pl.ds(at, SUB), :]
            off = left_off_ref[pl.ds(at, SUB), :]
            w = left_w_ref[pl.ds(at, SUB), :]
            for k in range(mine):
                base = k * span + REACH + half * SUB
                picked = None
                for o in range(width):
                    start = base + o - REACH
                    value = jnp.take_along_axis(
                        src[start : start + SUB, :], idx, axis=1, mode="promise_in_bounds"
                    )
                    picked = value if picked is None else jnp.where(off == o, value, picked)
                now = dst[base : base + SUB, :]
                halo_store(dst, k, half, groups, span, jnp.minimum(now, picked + w))


def sweep_pairs(count, mine, degree, first_over, one, two, tables):
    @pl.loop(0, count // 2)
    def _(_):
        sweep_once(mine, degree, first_over, one, two, tables)
        sweep_once(mine, degree, first_over, two, one, tables)


def begin_kernel(
    mine, degree, source_hbm, buf_ref, partner_ref,
    x_ref, idx_ref, w_ref, left_idx_ref, left_off_ref, left_w_ref, over_ref,
    stage, stage_tail, stage_w, source_ref, sems,
):
    (copy,) = fetch(((source_hbm, source_ref),), sems)
    pitch = stage.shape[0] // mine
    peers = 2 * buf_ref.shape[0]
    span = x_ref.shape[0] // mine
    block_total = span - PAD
    groups = block_total // SUB
    shard_blocks = block_total // peers
    arc_rows = degree * shard_blocks
    dist_rows = mine * shard_blocks
    even = lax.axis_index("arc") % 2 == 0

    def unpack(target, i, b, rows, own_at, partner_at):
        own = buf_ref[i, own_at + b * rows : own_at + (b + 1) * rows, :]
        partner = partner_ref[i, partner_at + b * rows : partner_at + (b + 1) * rows, :]
        blk = 2 * i * shard_blocks + b
        target[pl.ds(blk, rows, stride=pitch), :] = jnp.where(even, own, partner)
        blk = blk + shard_blocks
        target[pl.ds(blk, rows, stride=pitch), :] = jnp.where(even, partner, own)

    for i in range(peers // 2):
        for b in range(shard_blocks):
            unpack(stage, i, b, mine, 0, 2 * arc_rows)
            unpack(stage_tail, i, b, degree, dist_rows, 0)
            unpack(stage_w, i, b, degree, dist_rows + arc_rows, arc_rows)
    over = None
    for half in range(groups):
        part = plan_rounds(
            degree, block_total, half, stage_tail, stage_w, idx_ref, w_ref,
            left_idx_ref, left_off_ref, left_w_ref,
        )
        over = part if over is None else jnp.minimum(over, part)
    copy.wait()
    rows = lax.broadcasted_iota(jnp.int32, (SUB, LANES), 0)
    lanes = lax.broadcasted_iota(jnp.int32, (SUB, LANES), 1)
    first = lax.axis_index("arc") * mine
    for half in range(groups):
        node = (rows + half * SUB) * LANES + lanes
        for k in range(mine):
            at = k * pitch + half * SUB
            value = jnp.where(node == source_ref[first + k], jnp.float32(0.0), stage[at : at + SUB, :])
            halo_store(x_ref, k, half, groups, span, value)
    over_ref[...] = jnp.full(over_ref.shape, jnp.min(over.astype(jnp.float32)).astype(jnp.int32))


def merge_kernel(a_ref, b_ref, after_ref, *out_refs):
    total = a_ref[...] + b_ref[...]
    for n, ref in enumerate(out_refs):
        rows = ref.shape[0]
        ref[...] = total[n * rows : (n + 1) * rows, :]


def middle_kernel(
    mine, degree, count, over_ref, start_ref, idx_ref, w_ref, left_idx_ref, left_off_ref,
    left_w_ref, x_ref, other,
):
    x_ref[...] = start_ref[...]
    tables = (idx_ref, w_ref, left_idx_ref, left_off_ref, left_w_ref)
    sweep_pairs(count, mine, degree, over_ref[0, 0], x_ref, other, tables)


def end_kernel(
    mine, degree, count, parts, over_ref, start_ref, idx_ref, w_ref, left_idx_ref, left_off_ref,
    left_w_ref, cap_ref, *refs,
):
    flow_refs, (out_ref, grad_ref, x_ref, other) = refs[:parts], refs[parts:]
    peers = out_ref.shape[0]
    span = x_ref.shape[0] // mine
    block_total = span - PAD
    shard_blocks = block_total // peers
    tables = (idx_ref, w_ref, left_idx_ref, left_off_ref, left_w_ref)
    first_over = over_ref[0, 0]
    x_ref[...] = start_ref[...]
    if count:
        sweep_pairs(count, mine, degree, first_over, x_ref, other, tables)
    square = None
    for b in range(shard_blocks):
        cols = slice(b * LANES, (b + 1) * LANES)
        flow = None
        for ref in flow_refs:
            part = ref[b * degree : (b + 1) * degree, :]
            flow = part if flow is None else flow + part
        grad = flow - cap_ref[:, cols]
        grad_ref[:, cols] = grad
        term = grad * grad
        square = term if square is None else square + term
    folded = jnp.sum(square.reshape(degree // SUB, SUB, LANES), axis=0)
    base = mine * shard_blocks
    for i in range(peers):
        for b in range(shard_blocks):
            blk = REACH + i * shard_blocks + b
            out_ref[i, b * mine : (b + 1) * mine, :] = x_ref[pl.ds(blk, mine, stride=span), :]
        out_ref[i, base : base + SUB, :] = folded


def final_kernel(mine, arc_total, buf_ref, grad_ref, price_ref, dist_ref, new_ref):
    peers = buf_ref.shape[0]
    shard_blocks = dist_ref.shape[1] // LANES
    base = mine * shard_blocks
    total = None
    for i in range(peers):
        for b in range(shard_blocks):
            dist_ref[i * mine : (i + 1) * mine, b * LANES : (b + 1) * LANES] = buf_ref[
                i, b * mine : (b + 1) * mine, :
            ]
        part = buf_ref[i, base : base + SUB, :]
        total = part if total is None else total + part
    square_sum = jnp.sum(jnp.sum(total, axis=1, keepdims=True), axis=0, keepdims=True)
    scale_root = jnp.sqrt(square_sum / arc_total + eps_value)
    new_ref[...] = jnp.maximum(
        price_ref[...] + step_size * grad_ref[...] / scale_root, jnp.float32(0.0)
    )


def shards(prev_dist, source_node, arc_tail, base_cost, arc_price, capacity, path_arcs, demand):
    commodities, shard_nodes = prev_dist.shape
    peers = lax.axis_size("arc")
    groups = lax.axis_size("comm")
    node_count = shard_nodes * peers
    degree = arc_tail.shape[0]
    mine = commodities // peers
    shard_blocks = shard_nodes // LANES
    block_total = node_count // LANES
    span = block_total + PAD
    arc_rows = degree * shard_blocks
    f32, i32 = jnp.float32, jnp.int32
    shape = jax.ShapeDtypeStruct
    near = pltpu.VMEM
    v = vmem_spec

    def held(x):
        return pltpu.with_memory_space_constraint(x, pltpu.VMEM)

    def far(x):
        return pltpu.with_memory_space_constraint(x, pltpu.HBM)

    def scratch(*arrays):
        return [pltpu.VMEM(x.shape, x.dtype) for x in arrays]

    h = functools.partial(pl.BlockSpec, memory_space=pltpu.HBM)
    params = pltpu.CompilerParams(vmem_limit_bytes=VMEM_GRANT)
    arcs = (arc_tail, base_cost, arc_price, prev_dist)
    packed = pl.pallas_call(
        functools.partial(pack_kernel, node_count),
        out_shape=near((peers // 2, 2 * mine * shard_blocks + 4 * arc_rows, LANES), f32),
        in_specs=[h()] * 6,
        out_specs=v(),
        scratch_shapes=[
            *scratch(path_arcs),
            pltpu.SMEM(demand.shape, f32),
            *scratch(*arcs),
            pltpu.SemaphoreType.DMA((6,)),
        ],
        compiler_params=params,
        name="pack",
    )(far(path_arcs), far(demand), *map(far, arcs))
    parities = [list(range(side, peers, 2)) for side in range(2)]
    received = held(
        lax.all_to_all(packed, "arc", 0, 0, tiled=True, axis_index_groups=parities)
    )

    def swap(x):
        return held(lax.ppermute(x, "arc", [(i, i ^ 1) for i in range(peers)]))

    def exchange(x, step):
        pairs = [(i, i ^ (1 << step)) for i in range(groups)]
        return held(lax.ppermute(x, "comm", pairs))

    def merge(a, b, after, parts):
        return pl.pallas_call(
            merge_kernel,
            out_shape=(near((arc_rows, LANES), f32),) * parts,
            in_specs=[v(), v(), v()],
            out_specs=(v(),) * parts,
            compiler_params=params,
            name="merge",
        )(held(a), b, held(after))

    flow, passed = pl.pallas_call(
        split_kernel,
        out_shape=(
            near((2 * arc_rows, LANES), f32),
            near((peers // 2, 2 * arc_rows + mine * shard_blocks, LANES), f32),
        ),
        in_specs=[v()],
        out_specs=(v(), v()),
        compiler_params=params,
        name="split",
    )(received)
    partner = swap(held(passed))

    steps = groups.bit_length() - 1
    if 1 << steps != groups:
        flow, steps = held(lax.psum(flow, "comm")), 0
    arrived = exchange(flow, 0) if steps else jnp.zeros_like(flow)

    rounds = ROUNDS
    table = degree * block_total
    state = (mine * span, LANES)
    x, *tables, over = pl.pallas_call(
        functools.partial(begin_kernel, mine, degree),
        out_shape=(
            near(state, f32),
            near((rounds * block_total, LANES), i32),
            near((rounds * block_total, LANES), f32),
            near((table, LANES), i32),
            near((table, LANES), i32),
            near((table, LANES), f32),
            near((SUB, LANES), i32),
        ),
        in_specs=[h(), v(), v()],
        out_specs=(v(),) * 7,
        scratch_shapes=[
            pltpu.VMEM((mine * (block_total + 1), LANES), f32),
            pltpu.VMEM((degree * (block_total + 1), LANES), f32),
            pltpu.VMEM((degree * (block_total + 1), LANES), f32),
            pltpu.SMEM(source_node.shape, i32),
            pltpu.SemaphoreType.DMA((1,)),
        ],
        compiler_params=params,
        name="begin",
    )(far(source_node), received, partner)

    tables, over = tuple(map(held, tables)), held(over)
    def sweep(x, count):
        return pl.pallas_call(
            functools.partial(middle_kernel, mine, degree, count),
            out_shape=near(state, f32),
            in_specs=[v()] * (len(tables) + 2),
            out_specs=v(),
            scratch_shapes=[pltpu.VMEM(state, f32)],
            compiler_params=params,
            name="middle",
        )(over, held(x), *tables)

    x = sweep(x, 2)
    left = SWEEPS - 2
    flow, other = merge(flow, held(arrived), x, 2)
    arrived = swap(held(other))
    for step in range(1, max(steps, 1) + 1):
        count = min(2 if step < steps else 4, left)
        left -= count
        x = sweep(x, count)
        if step < steps:
            (flow,) = merge(flow, arrived, x, 1)
            arrived = exchange(held(flow), step)

    flows = (held(flow), arrived)
    back, gradient = pl.pallas_call(
        functools.partial(end_kernel, mine, degree, left, len(flows)),
        out_shape=(
            near((peers, mine * shard_blocks + SUB, LANES), f32),
            near((degree, shard_nodes), f32),
        ),
        in_specs=[v()] * (len(tables) + 3 + len(flows)),
        out_specs=(v(), v()),
        scratch_shapes=[pltpu.VMEM(state, f32), pltpu.VMEM(state, f32)],
        compiler_params=params,
        name="end",
    )(over, held(x), *tables, capacity, *flows)
    final = held(lax.all_to_all(back, "arc", 0, 0, tiled=True))
    return pl.pallas_call(
        functools.partial(final_kernel, mine, degree * node_count),
        out_shape=(shape((commodities, shard_nodes), f32), shape((degree, shard_nodes), f32)),
        in_specs=[v(), v(), v()],
        out_specs=(v(), v()),
        compiler_params=params,
        name="finish",
    )(final, held(gradient), arc_price)


def solution(mesh):
    in_specs = (
        P("comm", "arc"),
        P("comm"),
        P(None, "arc"),
        P(None, "arc"),
        P(None, "arc"),
        P(None, "arc"),
        P(("comm", "arc"), None),
        P(("comm", "arc")),
    )
    out_specs = (P("comm", "arc"), P(None, "arc"))
    return jax.shard_map(shards, mesh=mesh, in_specs=in_specs, out_specs=out_specs, check_vma=False)
```

```python
import functools

import jax
import jax.numpy as jnp
from jax import lax
from jax.experimental import pallas as pl
from jax.experimental.pallas import tpu as pltpu
from jax.sharding import PartitionSpec as P

SWEEPS = 8
REACH = 2
LANES = 128
SUB = 8
PAD = 2 * REACH + 1
VMEM_GRANT = 24 * 1024 * 1024

TURNS = ((None, None, 5), (0, 1, 5), (2, 3, 5), (4, 5, 5), (6, 0, 2))
ROUNDS = sum(turn[2] for turn in TURNS)

step_size = 0.25
eps_value = 1e-06


def vmem_spec():
    return pl.BlockSpec(memory_space=pltpu.VMEM)


def three_parts(x):
    first = x.astype(jnp.bfloat16)
    rest = x - first.astype(jnp.float32)
    second = rest.astype(jnp.bfloat16)
    third = (rest - second.astype(jnp.float32)).astype(jnp.bfloat16)
    return first, second, third


def fetch(pairs, sems):
    copies = [pltpu.make_async_copy(src, dst, sems.at[n]) for n, (src, dst) in enumerate(pairs)]
    for copy in copies:
        copy.start()
    return copies


def pack_kernel(
    node_count, path_hbm, demand_hbm, tail_hbm, cost_hbm, price_hbm, dist_hbm, out_ref,
    path_ref, demand_ref, tail_ref, cost_ref, price_ref, dist_ref, sems,
):
    copies = fetch(
        (
            (path_hbm, path_ref),
            (demand_hbm, demand_ref),
            (tail_hbm, tail_ref),
            (cost_hbm, cost_ref),
            (price_hbm, price_ref),
            (dist_hbm, dist_ref),
        ),
        sems,
    )
    peers = 2 * out_ref.shape[0]
    degree, shard_nodes = tail_ref.shape
    shard_blocks = shard_nodes // LANES
    mine = dist_ref.shape[0] // peers
    block_total = node_count // LANES
    routes, hops = path_ref.shape

    copies[0].wait()
    copies[1].wait()
    path = path_ref[...]
    slot = path // node_count
    node = path - slot * node_count
    block = node // LANES
    lane = node - block * LANES
    row = block * degree + slot
    row_total = block_total * degree
    row_ids = lax.broadcasted_iota(jnp.int32, (row_total, hops), 0)
    lane_ids = lax.broadcasted_iota(jnp.int32, (LANES, hops), 0)
    left = [[], [], []]
    right = []
    for k in range(routes):
        hit = row_ids == row[k : k + 1, :]
        amount = jnp.full((1, hops), demand_ref[k], jnp.float32)
        for part, piece in enumerate(three_parts(amount)):
            left[part].append(
                jnp.where(hit, piece.astype(jnp.float32), jnp.float32(0.0)).astype(jnp.bfloat16)
            )
        right.append(
            jnp.where(lane_ids == lane[k : k + 1, :], jnp.float32(1.0), jnp.float32(0.0)).astype(
                jnp.bfloat16
            )
        )
    right = jnp.concatenate(right, axis=1)
    flow = None
    for part in (2, 1, 0):
        term = lax.dot_general(
            jnp.concatenate(left[part], axis=1),
            right,
            (((1,), (1,)), ((), ())),
            preferred_element_type=jnp.float32,
        )
        flow = term if flow is None else flow + term

    for copy in copies[2:]:
        copy.wait()
    tail = tail_ref[...].astype(jnp.float32)
    weight = cost_ref[...] + price_ref[...]
    arc_rows = degree * shard_blocks
    dist_rows = mine * shard_blocks
    even = lax.axis_index("arc") % 2 == 0
    for pair in range(peers // 2):
        for b in range(shard_blocks):
            cols = slice(b * LANES, (b + 1) * LANES)
            first, second = (
                dist_ref[j * mine : (j + 1) * mine, cols] for j in (2 * pair, 2 * pair + 1)
            )
            at = b * mine
            out_ref[pair, at : at + mine, :] = jnp.where(even, first, second)
            at = dist_rows + b * degree
            out_ref[pair, at : at + degree, :] = tail[:, cols]
            at = at + arc_rows
            out_ref[pair, at : at + degree, :] = weight[:, cols]
            at = dist_rows + 2 * arc_rows + b * mine
            out_ref[pair, at : at + mine, :] = jnp.where(even, second, first)
        first, second = (
            flow[j * arc_rows : (j + 1) * arc_rows, :] for j in (2 * pair, 2 * pair + 1)
        )
        at = 2 * dist_rows + 2 * arc_rows
        out_ref[pair, at : at + arc_rows, :] = jnp.where(even, first, second)
        at = at + arc_rows
        out_ref[pair, at : at + arc_rows, :] = jnp.where(even, second, first)


def halo_store(ref, k, half, groups, span, value):
    blocks = groups * SUB
    base = k * span + REACH
    ref[base + half * SUB : base + (half + 1) * SUB, :] = value
    if half == groups - 1:
        ref[base - REACH : base, :] = value[SUB - REACH :, :]
    if half == 0:
        ref[base + blocks : base + blocks + REACH, :] = value[:REACH, :]


def split_kernel(buf_ref, flow_ref, pass_ref):
    total = None
    end = buf_ref.shape[1] - flow_ref.shape[0]
    for i in range(buf_ref.shape[0]):
        part = buf_ref[i, end:, :]
        total = part if total is None else total + part
        pass_ref[i, :, :] = buf_ref[i, end - pass_ref.shape[1] : end, :]
    flow_ref[...] = total


def plan_rounds(
    degree, block_total, half, stage, stage_w, idx_ref, w_ref, left_idx_ref, left_off_ref, left_w_ref
):
    groups = block_total // SUB
    width = 2 * REACH + 1
    rows = lax.broadcasted_iota(jnp.int32, (SUB, LANES), 0) + half * SUB
    used = jnp.zeros((SUB, LANES), jnp.int32)
    over = jnp.full((SUB, LANES), degree, jnp.int32)
    lanes_of, weights, bits, opens, offs = [], [], [], [], []
    for s in range(degree):
        at = s * (stage.shape[0] // degree) + half * SUB
        tail = stage[at : at + SUB, :].astype(jnp.int32)
        block = tail // LANES
        lane = tail - block * LANES
        off = block - rows + REACH
        off = jnp.where(off < 0, off + block_total, off)
        off = jnp.where(off >= block_total, off - block_total, off)
        weight = stage_w[at : at + SUB, :]
        turned = [jnp.left_shift(1, off)]
        for _ in range(3):
            last = turned[-1]
            turned.append(((last << 1) | (last >> (width - 1))) & (2**width - 1))
        open_rounds = jnp.zeros_like(used)
        for j, (low, high, count) in enumerate(TURNS):
            if low is None:
                spot = turned[0]
            else:
                by_low = ((lane >> low) & 1) == 1
                by_high = ((lane >> high) & 1) == 1
                spot = jnp.where(
                    by_high,
                    jnp.where(by_low, turned[3], turned[2]),
                    jnp.where(by_low, turned[1], turned[0]),
                )
            if count < width:
                spot = spot & (2**count - 1)
            open_rounds = open_rounds | (spot << (width * j))
        free = open_rounds & ~used
        bit = free & -free
        if s >= len(TURNS) - 1:
            near, far = jnp.zeros_like(used), jnp.zeros_like(used)
            for earlier, taken in zip(opens, bits):
                near = near | jnp.where((earlier & ~used) != 0, taken, 0)
            for earlier, taken in zip(opens, bits):
                far = far | jnp.where((earlier & near) != 0, taken, 0)
            straight = open_rounds & near
            wanted = jnp.where(straight != 0, straight, open_rounds & far)
            wanted = jnp.where(bit == 0, wanted & -wanted, 0)
            twice = jnp.where((straight != 0) | (wanted == 0), -1, wanted)
            passed = jnp.zeros_like(used)
            for earlier, taken in zip(opens, bits):
                passed = passed | jnp.where(taken == twice, earlier, 0)
            passed = passed & near
            passed = passed & -passed
            last = passed | jnp.where(straight != 0, wanted, 0)
            last = jnp.where(last == 0, -1, last)
            end = jnp.zeros_like(used)
            for earlier, taken in zip(opens, bits):
                end = end | jnp.where(taken == last, earlier, 0)
            end = end & ~used
            end = end & -end
            used = used | end
            for e, taken in enumerate(bits):
                bits[e] = jnp.where(taken == last, end, jnp.where(taken == twice, passed, taken))
            bit = bit | wanted
        used = used | bit
        over = jnp.minimum(over, jnp.where(bit == 0, s, degree))
        opens.append(open_rounds)
        offs.append(off)
        lanes_of.append(lane)
        weights.append(weight)
        bits.append(bit)
    for s in range(degree):
        at = s * block_total + half * SUB
        left_idx_ref[at : at + SUB, :] = lanes_of[s]
        left_off_ref[at : at + SUB, :] = offs[s]
        left_w_ref[at : at + SUB, :] = jnp.where(bits[s] == 0, weights[s], jnp.float32(jnp.inf))
    for r in range(ROUNDS):
        idx = jnp.zeros((SUB, LANES), jnp.int32)
        weight = jnp.full((SUB, LANES), jnp.inf, jnp.float32)
        for s in range(degree):
            hit = bits[s] == (1 << r)
            idx = jnp.where(hit, lanes_of[s], idx)
            weight = jnp.where(hit, weights[s], weight)
        at = (r * groups + half) * SUB
        idx_ref[at : at + SUB, :] = idx
        w_ref[at : at + SUB, :] = weight
    return over


def sweep_once(mine, degree, first_over, src, dst, tables):
    idx_ref, w_ref, left_idx_ref, left_off_ref, left_w_ref = tables
    span = src.shape[0] // mine
    block_total = span - PAD
    groups = block_total // SUB
    width = 2 * REACH + 1
    lane = lax.broadcasted_iota(jnp.int32, (SUB, LANES), 1)
    bit_masks = [((lane >> t) & 1) == 1 for t in range(LANES.bit_length() - 1)]
    for half in range(groups):
        best = [src[k * span + REACH + half * SUB : k * span + REACH + (half + 1) * SUB, :] for k in range(mine)]
        for j, (low, high, count) in enumerate(TURNS):
            for q in range(count):
                at = ((j * width + q) * groups + half) * SUB
                idx = idx_ref[at : at + SUB, :]
                w = w_ref[at : at + SUB, :]
                for k in range(mine):
                    base = k * span + half * SUB

                    def block(turned):
                        o = base + (q - turned) % width
                        return src[o : o + SUB, :]

                    if low is None:
                        shown = block(0)
                    else:
                        shown = jnp.where(
                            bit_masks[high],
                            jnp.where(bit_masks[low], block(3), block(2)),
                            jnp.where(bit_masks[low], block(1), block(0)),
                        )
                    value = jnp.take_along_axis(shown, idx, axis=1, mode="promise_in_bounds")
                    best[k] = jnp.minimum(best[k], value + w)
        for k in range(mine):
            halo_store(dst, k, half, groups, span, best[k])

    @pl.loop(first_over, degree)
    def _(s):
        for half in range(groups):
            at = pl.multiple_of(s * block_total + half * SUB, SUB)
            idx = left_idx_ref[pl.ds(at, SUB), :]
            off = left_off_ref[pl.ds(at, SUB), :]
            w = left_w_ref[pl.ds(at, SUB), :]
            for k in range(mine):
                base = k * span + REACH + half * SUB
                picked = None
                for o in range(width):
                    start = base + o - REACH
                    value = jnp.take_along_axis(
                        src[start : start + SUB, :], idx, axis=1, mode="promise_in_bounds"
                    )
                    picked = value if picked is None else jnp.where(off == o, value, picked)
                now = dst[base : base + SUB, :]
                halo_store(dst, k, half, groups, span, jnp.minimum(now, picked + w))


def sweep_pairs(count, mine, degree, first_over, one, two, tables):
    @pl.loop(0, count // 2)
    def _(_):
        sweep_once(mine, degree, first_over, one, two, tables)
        sweep_once(mine, degree, first_over, two, one, tables)


def begin_kernel(
    mine, degree, source_hbm, buf_ref, partner_ref,
    x_ref, idx_ref, w_ref, left_idx_ref, left_off_ref, left_w_ref, over_ref,
    stage, stage_tail, stage_w, source_ref, sems,
):
    (copy,) = fetch(((source_hbm, source_ref),), sems)
    pitch = stage.shape[0] // mine
    peers = 2 * buf_ref.shape[0]
    span = x_ref.shape[0] // mine
    block_total = span - PAD
    groups = block_total // SUB
    shard_blocks = block_total // peers
    arc_rows = degree * shard_blocks
    dist_rows = mine * shard_blocks
    even = lax.axis_index("arc") % 2 == 0

    def unpack(target, i, b, rows, own_at, partner_at):
        own = buf_ref[i, own_at + b * rows : own_at + (b + 1) * rows, :]
        partner = partner_ref[i, partner_at + b * rows : partner_at + (b + 1) * rows, :]
        blk = 2 * i * shard_blocks + b
        target[pl.ds(blk, rows, stride=pitch), :] = jnp.where(even, own, partner)
        blk = blk + shard_blocks
        target[pl.ds(blk, rows, stride=pitch), :] = jnp.where(even, partner, own)

    for i in range(peers // 2):
        for b in range(shard_blocks):
            unpack(stage, i, b, mine, 0, 2 * arc_rows)
            unpack(stage_tail, i, b, degree, dist_rows, 0)
            unpack(stage_w, i, b, degree, dist_rows + arc_rows, arc_rows)
    over = None
    for half in range(groups):
        part = plan_rounds(
            degree, block_total, half, stage_tail, stage_w, idx_ref, w_ref,
            left_idx_ref, left_off_ref, left_w_ref,
        )
        over = part if over is None else jnp.minimum(over, part)
    copy.wait()
    rows = lax.broadcasted_iota(jnp.int32, (SUB, LANES), 0)
    lanes = lax.broadcasted_iota(jnp.int32, (SUB, LANES), 1)
    first = lax.axis_index("arc") * mine
    for half in range(groups):
        node = (rows + half * SUB) * LANES + lanes
        for k in range(mine):
            at = k * pitch + half * SUB
            value = jnp.where(node == source_ref[first + k], jnp.float32(0.0), stage[at : at + SUB, :])
            halo_store(x_ref, k, half, groups, span, value)
    over_ref[...] = jnp.full(over_ref.shape, jnp.min(over.astype(jnp.float32)).astype(jnp.int32))


def merge_kernel(a_ref, b_ref, after_ref, *out_refs):
    total = a_ref[...] + b_ref[...]
    for n, ref in enumerate(out_refs):
        rows = ref.shape[0]
        ref[...] = total[n * rows : (n + 1) * rows, :]


def middle_kernel(
    mine, degree, count, over_ref, start_ref, idx_ref, w_ref, left_idx_ref, left_off_ref,
    left_w_ref, x_ref, other,
):
    x_ref[...] = start_ref[...]
    tables = (idx_ref, w_ref, left_idx_ref, left_off_ref, left_w_ref)
    sweep_pairs(count, mine, degree, over_ref[0, 0], x_ref, other, tables)


def end_kernel(
    mine, degree, count, parts, over_ref, start_ref, idx_ref, w_ref, left_idx_ref, left_off_ref,
    left_w_ref, cap_ref, *refs,
):
    flow_refs, (out_ref, grad_ref, x_ref, other) = refs[:parts], refs[parts:]
    peers = out_ref.shape[0]
    span = x_ref.shape[0] // mine
    block_total = span - PAD
    shard_blocks = block_total // peers
    tables = (idx_ref, w_ref, left_idx_ref, left_off_ref, left_w_ref)
    first_over = over_ref[0, 0]
    if count:
        x_ref[...] = start_ref[...]
        sweep_pairs(count, mine, degree, first_over, x_ref, other, tables)
    else:
        x_ref = start_ref
    square = None
    for b in range(shard_blocks):
        cols = slice(b * LANES, (b + 1) * LANES)
        flow = None
        for ref in flow_refs:
            part = ref[b * degree : (b + 1) * degree, :]
            flow = part if flow is None else flow + part
        grad = flow - cap_ref[:, cols]
        grad_ref[:, cols] = grad
        term = grad * grad
        square = term if square is None else square + term
    folded = jnp.sum(square.reshape(degree // SUB, SUB, LANES), axis=0)
    base = mine * shard_blocks
    for i in range(peers):
        for b in range(shard_blocks):
            blk = REACH + i * shard_blocks + b
            out_ref[i, b * mine : (b + 1) * mine, :] = x_ref[pl.ds(blk, mine, stride=span), :]
        out_ref[i, base : base + SUB, :] = folded


def final_kernel(mine, arc_total, buf_ref, grad_ref, price_ref, dist_ref, new_ref):
    peers = buf_ref.shape[0]
    shard_blocks = dist_ref.shape[1] // LANES
    base = mine * shard_blocks
    total = None
    for i in range(peers):
        for b in range(shard_blocks):
            dist_ref[i * mine : (i + 1) * mine, b * LANES : (b + 1) * LANES] = buf_ref[
                i, b * mine : (b + 1) * mine, :
            ]
        part = buf_ref[i, base : base + SUB, :]
        total = part if total is None else total + part
    square_sum = jnp.sum(jnp.sum(total, axis=1, keepdims=True), axis=0, keepdims=True)
    scale_root = jnp.sqrt(square_sum / arc_total + eps_value)
    new_ref[...] = jnp.maximum(
        price_ref[...] + step_size * grad_ref[...] / scale_root, jnp.float32(0.0)
    )


def shards(prev_dist, source_node, arc_tail, base_cost, arc_price, capacity, path_arcs, demand):
    commodities, shard_nodes = prev_dist.shape
    peers = lax.axis_size("arc")
    groups = lax.axis_size("comm")
    node_count = shard_nodes * peers
    degree = arc_tail.shape[0]
    mine = commodities // peers
    shard_blocks = shard_nodes // LANES
    block_total = node_count // LANES
    span = block_total + PAD
    arc_rows = degree * shard_blocks
    f32, i32 = jnp.float32, jnp.int32
    shape = jax.ShapeDtypeStruct
    near = pltpu.VMEM
    v = vmem_spec

    def held(x):
        return pltpu.with_memory_space_constraint(x, pltpu.VMEM)

    def far(x):
        return pltpu.with_memory_space_constraint(x, pltpu.HBM)

    def scratch(*arrays):
        return [pltpu.VMEM(x.shape, x.dtype) for x in arrays]

    h = functools.partial(pl.BlockSpec, memory_space=pltpu.HBM)
    params = pltpu.CompilerParams(vmem_limit_bytes=VMEM_GRANT)
    arcs = (arc_tail, base_cost, arc_price, prev_dist)
    packed = pl.pallas_call(
        functools.partial(pack_kernel, node_count),
        out_shape=near((peers // 2, 2 * mine * shard_blocks + 4 * arc_rows, LANES), f32),
        in_specs=[h()] * 6,
        out_specs=v(),
        scratch_shapes=[
            *scratch(path_arcs),
            pltpu.SMEM(demand.shape, f32),
            *scratch(*arcs),
            pltpu.SemaphoreType.DMA((6,)),
        ],
        compiler_params=params,
        name="pack",
    )(far(path_arcs), far(demand), *map(far, arcs))
    parities = [list(range(side, peers, 2)) for side in range(2)]
    received = held(
        lax.all_to_all(packed, "arc", 0, 0, tiled=True, axis_index_groups=parities)
    )

    def swap(x):
        return held(lax.ppermute(x, "arc", [(i, i ^ 1) for i in range(peers)]))

    def exchange(x, step):
        pairs = [(i, i ^ (1 << step)) for i in range(groups)]
        return held(lax.ppermute(x, "comm", pairs))

    def merge(a, b, after, parts):
        return pl.pallas_call(
            merge_kernel,
            out_shape=(near((arc_rows, LANES), f32),) * parts,
            in_specs=[v(), v(), v()],
            out_specs=(v(),) * parts,
            compiler_params=params,
            name="merge",
        )(held(a), b, held(after))

    flow, passed = pl.pallas_call(
        split_kernel,
        out_shape=(
            near((2 * arc_rows, LANES), f32),
            near((peers // 2, 2 * arc_rows + mine * shard_blocks, LANES), f32),
        ),
        in_specs=[v()],
        out_specs=(v(), v()),
        compiler_params=params,
        name="split",
    )(received)
    partner = swap(held(passed))

    steps = groups.bit_length() - 1
    if 1 << steps != groups:
        flow, steps = held(lax.psum(flow, "comm")), 0
    arrived = exchange(flow, 0) if steps else jnp.zeros_like(flow)

    rounds = ROUNDS
    table = degree * block_total
    state = (mine * span, LANES)
    x, *tables, over = pl.pallas_call(
        functools.partial(begin_kernel, mine, degree),
        out_shape=(
            near(state, f32),
            near((rounds * block_total, LANES), i32),
            near((rounds * block_total, LANES), f32),
            near((table, LANES), i32),
            near((table, LANES), i32),
            near((table, LANES), f32),
            near((SUB, LANES), i32),
        ),
        in_specs=[h(), v(), v()],
        out_specs=(v(),) * 7,
        scratch_shapes=[
            pltpu.VMEM((mine * (block_total + 1), LANES), f32),
            pltpu.VMEM((degree * (block_total + 1), LANES), f32),
            pltpu.VMEM((degree * (block_total + 1), LANES), f32),
            pltpu.SMEM(source_node.shape, i32),
            pltpu.SemaphoreType.DMA((1,)),
        ],
        compiler_params=params,
        name="begin",
    )(far(source_node), received, partner)

    tables, over = tuple(map(held, tables)), held(over)
    def sweep(x, count):
        return pl.pallas_call(
            functools.partial(middle_kernel, mine, degree, count),
            out_shape=near(state, f32),
            in_specs=[v()] * (len(tables) + 2),
            out_specs=v(),
            scratch_shapes=[pltpu.VMEM(state, f32)],
            compiler_params=params,
            name="middle",
        )(over, held(x), *tables)

    x = sweep(x, 2)
    left = SWEEPS - 2
    flow, other = merge(flow, held(arrived), x, 2)
    arrived = swap(held(other))
    for step in range(1, max(steps, 1) + 1):
        count = min(2 if step < steps else 4, left)
        left -= count
        x = sweep(x, count)
        if step < steps:
            (flow,) = merge(flow, arrived, x, 1)
            arrived = exchange(held(flow), step)

    flows = (held(flow), arrived)
    back, gradient = pl.pallas_call(
        functools.partial(end_kernel, mine, degree, left, len(flows)),
        out_shape=(
            near((peers, mine * shard_blocks + SUB, LANES), f32),
            near((degree, shard_nodes), f32),
        ),
        in_specs=[v()] * (len(tables) + 3 + len(flows)),
        out_specs=(v(), v()),
        scratch_shapes=[pltpu.VMEM(state, f32), pltpu.VMEM(state, f32)],
        compiler_params=params,
        name="end",
    )(over, held(x), *tables, capacity, *flows)
    final = held(lax.all_to_all(back, "arc", 0, 0, tiled=True))
    return pl.pallas_call(
        functools.partial(final_kernel, mine, degree * node_count),
        out_shape=(shape((commodities, shard_nodes), f32), shape((degree, shard_nodes), f32)),
        in_specs=[v(), v(), v()],
        out_specs=(v(), v()),
        compiler_params=params,
        name="finish",
    )(final, held(gradient), arc_price)


def solution(mesh):
    in_specs = (
        P("comm", "arc"),
        P("comm"),
        P(None, "arc"),
        P(None, "arc"),
        P(None, "arc"),
        P(None, "arc"),
        P(("comm", "arc"), None),
        P(("comm", "arc")),
    )
    out_specs = (P("comm", "arc"), P(None, "arc"))
    return jax.shard_map(shards, mesh=mesh, in_specs=in_specs, out_specs=out_specs, check_vma=False)
```
